32 devices in a mesh: dp: 1 (over z), tp: 4 (over y), pp: 8 (over x, core).
Axes of the slice: x: 4, y: 4, z: 1, core: 2. Of those that a mesh axis runs over, the one named last changes fastest.
The devices are a block of a 4x4x8 slice.
Arguments:
- x_in: bfloat16 [16, 1, 128, 2560], P('dp', None, 'tp')
- ln1_gain: float32 [8, 2560], P('pp')
- ln1_shift: float32 [8, 2560], P('pp')
- w_qkv: bfloat16 [8, 2560, 7680], P('pp', None, 'tp')
- b_qkv: float32 [8, 7680], P('pp', 'tp')
- w_out: bfloat16 [8, 32, 80, 2560], P('pp', 'tp')
- b_out: float32 [8, 2560], P('pp')
- ln2_gain: float32 [8, 2560], P('pp')
- ln2_shift: float32 [8, 2560], P('pp')
- w_up: bfloat16 [8, 2560, 10240], P('pp', None, 'tp')
- b_up: float32 [8, 10240], P('pp', 'tp')
- w_down: bfloat16 [8, 10240, 2560], P('pp', 'tp')
- b_down: float32 [8, 2560], P('pp')
Outputs:
- output: bfloat16 [16, 1, 128, 2560], P(('dp', 'pp'), None, 'tp')
All inputs are finite; a program needn't handle non-finite values.
Results may differ from the reference program's by a relative error of at most 0.02.
Values are sent between devices in bfloat16 or wider.
A program may use at most 768 MiB of HBM per device.

```python
import jax
import jax.numpy as jnp
from jax import lax

NUM_MICRO = 16
BATCH_SIZE = 1
SEQ_LEN = 128
D_MODEL = 2560
NUM_HEADS = 32
D_FF = 10240
NUM_LAYERS = 8

HEAD_DIM = D_MODEL // NUM_HEADS
LN_EPS = 1e-5


def make_weight(rng_key, out_shape, fan_in):
    return (jax.random.normal(rng_key, out_shape, jnp.float32) * fan_in ** -0.5).astype(jnp.bfloat16)


def make_vector(rng_key, out_shape, center):
    return center + 0.25 * jax.random.normal(rng_key, out_shape, jnp.float32)


def setup_inputs(seed: int = 0, part: int = 0) -> dict:
    key_list = jax.random.split(jax.random.key(seed), 13)
    act_key = jax.random.fold_in(key_list[0], part)
    layers = NUM_LAYERS
    width = D_MODEL
    x_in = jax.random.normal(act_key, (NUM_MICRO, BATCH_SIZE, SEQ_LEN, width), jnp.float32)
    return {
        "x_in": x_in.astype(jnp.bfloat16),
        "ln1_gain": make_vector(key_list[1], (layers, width), 1.0),
        "ln1_shift": make_vector(key_list[2], (layers, width), 0.0),
        "w_qkv": make_weight(key_list[3], (layers, width, 3 * width), width),
        "b_qkv": make_vector(key_list[4], (layers, 3 * width), 0.0),
        "w_out": make_weight(key_list[5], (layers, NUM_HEADS, HEAD_DIM, width), width),
        "b_out": make_vector(key_list[6], (layers, width), 0.0),
        "ln2_gain": make_vector(key_list[7], (layers, width), 1.0),
        "ln2_shift": make_vector(key_list[8], (layers, width), 0.0),
        "w_up": make_weight(key_list[9], (layers, width, D_FF), width),
        "b_up": make_vector(key_list[10], (layers, D_FF), 0.0),
        "w_down": make_weight(key_list[11], (layers, D_FF, width), D_FF),
        "b_down": make_vector(key_list[12], (layers, width), 0.0),
    }


def layer_norm(act_rows, ln_gain, ln_shift):
    rows_f32 = act_rows.astype(jnp.float32)
    row_mean = jnp.mean(rows_f32, axis=-1, keepdims=True)
    centered = rows_f32 - row_mean
    row_var = jnp.mean(centered * centered, axis=-1, keepdims=True)
    return (centered * lax.rsqrt(row_var + LN_EPS) * ln_gain + ln_shift).astype(jnp.bfloat16)


def causal_attention(qkv_heads):
    by_head = jnp.moveaxis(qkv_heads, 2, 0)
    positions = jnp.arange(SEQ_LEN)
    causal = positions[:, None] >= positions[None, :]

    def one_head(head_block):
        q_head = head_block[:, :, 0].astype(jnp.float32)
        k_head = head_block[:, :, 1].astype(jnp.float32)
        v_head = head_block[:, :, 2].astype(jnp.float32)
        scores = jnp.einsum("bqe,bke->bqk", q_head, k_head) * HEAD_DIM ** -0.5
        scores = jnp.where(causal, scores, -1e30)
        attn_probs = jax.nn.softmax(scores, axis=-1).astype(jnp.bfloat16).astype(jnp.float32)
        return jnp.einsum("bqk,bke->bqe", attn_probs, v_head).astype(jnp.bfloat16)

    context = lax.map(one_head, by_head)
    return jnp.moveaxis(context, 0, 2)


def one_layer(act_in, layer_params):
    (ln1_gain, ln1_shift, w_qkv, b_qkv, w_out, b_out,
     ln2_gain, ln2_shift, w_up, b_up, w_down, b_down) = layer_params
    tokens = BATCH_SIZE * SEQ_LEN
    act_rows = act_in.reshape(tokens, D_MODEL)
    normed = layer_norm(act_rows, ln1_gain, ln1_shift)
    qkv = (jnp.dot(normed, w_qkv, preferred_element_type=jnp.float32) + b_qkv).astype(jnp.bfloat16)
    context = causal_attention(qkv.reshape(BATCH_SIZE, SEQ_LEN, NUM_HEADS, 3, HEAD_DIM))
    attn_out = jnp.dot(context.reshape(tokens, D_MODEL), w_out.reshape(D_MODEL, D_MODEL),
                       preferred_element_type=jnp.float32).astype(jnp.bfloat16)
    mid_act = (act_rows.astype(jnp.float32) + attn_out.astype(jnp.float32) + b_out).astype(jnp.bfloat16)
    normed_mid = layer_norm(mid_act, ln2_gain, ln2_shift)
    hidden = jax.nn.relu(jnp.dot(normed_mid, w_up, preferred_element_type=jnp.float32) + b_up).astype(jnp.bfloat16)
    down_out = jnp.dot(hidden, w_down, preferred_element_type=jnp.float32).astype(jnp.bfloat16)
    new_rows = (mid_act.astype(jnp.float32) + down_out.astype(jnp.float32) + b_down).astype(jnp.bfloat16)
    return new_rows.reshape(BATCH_SIZE, SEQ_LEN, D_MODEL)


def reference(x_in, ln1_gain, ln1_shift, w_qkv, b_qkv, w_out, b_out,
              ln2_gain, ln2_shift, w_up, b_up, w_down, b_down):
    stacked = (ln1_gain, ln1_shift, w_qkv, b_qkv, w_out, b_out,
               ln2_gain, ln2_shift, w_up, b_up, w_down, b_down)

    def run_micro(micro_act):
        def scan_step(layer_act, layer_params):
            return one_layer(layer_act, layer_params), None
        return lax.scan(scan_step, micro_act, stacked)[0]

    return lax.map(run_micro, x_in)
```

```python
import functools

import jax
import jax.numpy as jnp
from jax import lax
from jax.experimental import pallas as pl
from jax.experimental.pallas import tpu as pltpu
from jax.sharding import PartitionSpec as P

LN_EPS = 1e-5
MESH = pl.DeviceIdType.MESH
F32 = jnp.float32
BF16 = jnp.bfloat16


def norm_rows(rows, gain, shift):
    rows = rows.astype(F32)
    centered = rows - jnp.mean(rows, axis=-1, keepdims=True)
    var = jnp.mean(centered * centered, axis=-1, keepdims=True)
    return (centered * lax.rsqrt(var + LN_EPS) * gain + shift).astype(BF16)


def layer_kernel(
    num_stages, ring, head_dim,
    x_hbm, g1_ref, s1_ref, wqkv_hbm, bqkv_ref, wout_hbm, bout_ref,
    g2_ref, s2_ref, wup_hbm, bup_ref, wdn_hbm, bdn_ref,
    out_ref,
    wqkv, wout, wup, wdn,
    xs, xf, nb, qkv, cf, acc, x1, hid, part, rl_in, rl_out, fin, x2, obuf,
    w_sem, wg_send, wg_recv, xs_sem, ax_send, ax_recv, ac_send, ac_recv,
    rs_send, rs_recv, pp_send, o_sem, turn_sem,
):
    num_micro, shard, width = x_hbm.shape
    seq = shard * ring
    per_stage = num_micro // num_stages
    own_k = wout_hbm.shape[0]
    qkv_w = wqkv_hbm.shape[1]
    heads = own_k // head_dim
    half = width // 2
    last = num_stages - 1

    me = lax.axis_index("tp")
    stage = lax.axis_index("pp")
    right = lax.rem(me + 1, ring)
    left = lax.rem(me + ring - 1, ring)
    opp = lax.rem(me + 2, ring)
    to_right, to_left = {"tp": right}, {"tp": left}

    def rows_of(owner, n):
        return pl.ds(pl.multiple_of(owner * n, n), n)

    barrier = pltpu.get_barrier_semaphore()

    def greet(device):
        pl.semaphore_signal(barrier, inc=1, device_id=device, device_id_type=MESH)

    greet(to_right)
    greet(to_left)
    pl.when(stage > 0)(lambda: greet({"pp": stage - 1}))
    pl.when(stage < last)(lambda: greet({"pp": stage + 1}))
    pl.when(stage < last - 1)(lambda: greet({"pp": last}))

    @pl.when(stage == last)
    def _():
        for q in range(last - 1):
            greet({"pp": q})

    own_rows = rows_of(me, own_k)
    load_out = pltpu.make_async_copy(wout_hbm, wout.at[own_rows], w_sem.at[0])
    load_qkv = pltpu.make_async_copy(wqkv_hbm, wqkv, w_sem.at[1])
    load_up = pltpu.make_async_copy(wup_hbm, wup, w_sem.at[2])
    load_dn = pltpu.make_async_copy(wdn_hbm, wdn, w_sem.at[3])
    load_out.start()

    def load_x(i):
        return pltpu.make_async_copy(x_hbm.at[i], xs.at[i], xs_sem.at[i])

    @pl.when(stage == 0)
    def _():
        lax.fori_loop(0, num_micro, lambda i, c: (load_x(i).start(), c)[1], 0)

    load_qkv.start()
    load_up.start()
    load_dn.start()

    n_greet = (
        2
        + jnp.where(stage > 0, 1, 0)
        + jnp.where(stage < last, 1, 0)
        + jnp.where(stage < last - 1, 1, 0)
        + jnp.where(stage == last, last - 1, 0)
    )
    pl.semaphore_wait(barrier, n_greet)

    class Gather:
        def __init__(self, own, piece, send, recv):
            self.own, self.piece, self.send, self.recv = own, piece, send, recv

        def copy(self, k, src, owner, h, device):
            return pltpu.make_async_remote_copy(
                src_ref=src, dst_ref=self.piece(owner, h),
                send_sem=self.send.at[k], recv_sem=self.recv.at[k],
                device_id=device, device_id_type=MESH,
            )

        def hop1(self):
            return [
                self.copy(0, self.own(0), me, 0, to_right),
                self.copy(3, self.own(1), me, 1, to_left),
                self.copy(1, self.own(1), me, 1, to_right),
                self.copy(2, self.own(0), me, 0, to_left),
            ]

        def start(self):
            for c in self.hop1():
                c.start()

        def fwd(self):
            return (
                self.copy(4, self.piece(left, 0), left, 0, to_right),
                self.copy(5, self.piece(right, 1), right, 1, to_left),
            )

        def recv_wait(self, k, owner, h):
            self.copy(k, self.piece(owner, h), owner, h, to_right).wait_recv()

        def forward(self):
            a, b = self.fwd()
            self.recv_wait(0, left, 0)
            a.start()
            self.recv_wait(3, right, 1)
            b.start()

        def near(self):
            self.recv_wait(1, left, 1)
            self.recv_wait(2, right, 0)

        def far(self):
            self.recv_wait(4, opp, 0)
            self.recv_wait(5, opp, 1)
            for c in self.hop1():
                c.wait_send()
            for c in self.fwd():
                c.wait_send()

    wk = own_k // 2

    def w_piece(owner, h):
        return wout.at[pl.ds(pl.multiple_of(owner * own_k + h * wk, wk), wk)]

    gather_w = Gather(lambda h: w_piece(me, h), w_piece, wg_send, wg_recv)

    xh = shard // 2
    ch = seq // 2

    def gather_x(i):
        slot = lax.rem(i, 2)

        def piece(owner, h):
            return xf.at[slot, pl.ds(pl.multiple_of(owner * shard + h * xh, xh), xh)]

        def own(h):
            return xs.at[i, pl.ds(h * xh, xh)]

        return Gather(own, piece, ax_send.at[slot], ax_recv.at[slot])

    def gather_c(i):
        slot = lax.rem(i, 2)

        def piece(owner, h):
            return cf.at[slot, owner, pl.ds(h * ch, ch)]

        return Gather(lambda h: piece(me, h), piece, ac_send.at[slot], ac_recv.at[slot])

    def scatter(i):
        slot = lax.rem(i, 2)

        def mine(owner, h):
            return part.at[slot, rows_of(owner, shard), pl.ds(h * half, half)]

        def copy(k, src, dst, device):
            return pltpu.make_async_remote_copy(
                src_ref=src, dst_ref=dst, send_sem=rs_send.at[slot, k], recv_sem=rs_recv.at[slot, k],
                device_id=device, device_id_type=MESH,
            )

        first = [
            copy(0, mine(opp, 0), rl_in.at[slot, 0], to_right),
            copy(1, mine(opp, 1), rl_in.at[slot, 1], to_left),
            copy(2, mine(right, 1), fin.at[slot, 0], to_right),
            copy(3, mine(left, 0), fin.at[slot, 1], to_left),
        ]
        second = [
            copy(4, rl_out.at[slot, 0], fin.at[slot, 2], to_right),
            copy(5, rl_out.at[slot, 1], fin.at[slot, 3], to_left),
        ]
        return slot, mine, first, second

    def scatter_start(i):
        for c in scatter(i)[2]:
            c.start()

    def scatter_relay(i):
        slot, mine, first, second = scatter(i)
        for h, owner in ((0, right), (1, left)):
            first[h].wait_recv()
            rl_out[slot, h] = (rl_in[slot, h].astype(F32) + mine(owner, h)[...].astype(F32)).astype(BF16)
            second[h].start()

    def scatter_finish(i):
        slot, mine, first, second = scatter(i)
        first[2].wait_recv()
        first[3].wait_recv()
        second[0].wait_recv()
        second[1].wait_recv()
        sums = []
        for h, (a, b) in ((0, (1, 2)), (1, (0, 3))):
            sums.append(mine(me, h)[...].astype(F32) + fin[slot, a].astype(F32) + fin[slot, b].astype(F32))
        for c in (*first, *second):
            c.wait_send()
        return sums

    def x_arrival(i):
        load_x(i).wait()

    def ln_shard(i, owner):
        at = rows_of(owner, shard)
        nb[at] = norm_rows(xf[lax.rem(i, 2), at], g1_ref[...], s1_ref[...])

    row_pos = lax.broadcasted_iota(jnp.int32, (seq, seq), 0)
    col_pos = lax.broadcasted_iota(jnp.int32, (seq, seq), 1)
    causal = row_pos >= col_pos

    def attention_part(i):
        slot = lax.rem(i, 2)
        gx = gather_x(i)
        xf[slot, rows_of(me, shard)] = xs[i]
        ln_shard(i, me)
        gx.near()
        ln_shard(i, left)
        ln_shard(i, right)
        gx.far()
        ln_shard(i, opp)
        for lo, hi in ((0, 768), (768, 1536), (1536, qkv_w)):
            got = jnp.dot(nb[...], wqkv[:, lo:hi], preferred_element_type=F32)
            qkv[:, lo:hi] = (got + bqkv_ref[:, lo:hi]).astype(BF16)
        outs = []
        for n in range(heads):
            at = 3 * head_dim * n
            q = qkv[:, at : at + head_dim]
            k = qkv[:, at + head_dim : at + 2 * head_dim]
            v = qkv[:, at + 2 * head_dim : at + 3 * head_dim]
            scores = lax.dot_general(q, k, (((1,), (1,)), ((), ())), preferred_element_type=F32) * head_dim**-0.5
            scores = jnp.where(causal, scores, -1e30)
            e = jnp.exp(scores - jnp.max(scores, axis=-1, keepdims=True))
            probs = (e / jnp.sum(e, axis=-1, keepdims=True)).astype(BF16)
            outs.append(jnp.dot(probs, v, preferred_element_type=F32).astype(BF16))
        cf[slot, me] = jnp.concatenate(outs, axis=-1)
        gather_c(i).start()

    chunk = 512
    n_chunks = width // chunk

    def over_columns(f):
        def body(n, c):
            f(pl.ds(pl.multiple_of(n * chunk, chunk), chunk))
            return c

        lax.fori_loop(0, n_chunks, body, 0)

    def out_block(i, owner, first):
        slot = lax.rem(i, 2)

        def f(cols):
            got = jnp.dot(cf[slot, owner], wout[rows_of(owner, own_k), cols], preferred_element_type=F32)
            acc[:, cols] = got if first else acc[:, cols] + got

        over_columns(f)

    def mlp_first(i):
        slot = lax.rem(i, 2)
        gc = gather_c(i)
        gc.near()
        out_block(i, left, False)
        out_block(i, right, False)
        gc.far()

        def f(cols):
            got = jnp.dot(cf[slot, opp], wout[rows_of(opp, own_k), cols], preferred_element_type=F32)
            a = (acc[:, cols] + got).astype(BF16).astype(F32)
            x1[:, cols] = (xf[slot, :, cols].astype(F32) + a + bout_ref[:, cols]).astype(BF16)

        over_columns(f)

        def ln2(r, c):
            at = rows_of(r, shard)
            nb[at] = norm_rows(x1[at], g2_ref[...], s2_ref[...])
            return c

        lax.fori_loop(0, ring, ln2, 0)

        def up(cols):
            got = jnp.dot(nb[...], wup[:, cols], preferred_element_type=F32) + bup_ref[:, cols]
            hid[:, cols] = jnp.maximum(got, 0.0).astype(BF16)

        over_columns(up)

    def mlp_second(i):
        slot = lax.rem(i, 2)

        def down(cols):
            part[slot, :, cols] = jnp.dot(hid[...], wdn[:, cols], preferred_element_type=F32).astype(BF16)

        over_columns(down)
        scatter_start(i)

    def remote_out(i):
        return (stage < last) | (i < per_stage * last)

    def next_copy(i):
        slot = lax.rem(i, 2)
        return pltpu.make_async_remote_copy(
            src_ref=x2.at[slot], dst_ref=xs.at[i], send_sem=pp_send.at[slot], recv_sem=xs_sem.at[i],
            device_id={"pp": lax.rem(stage + 1, num_stages)}, device_id_type=MESH,
        )

    def out_copy(i):
        slot = lax.rem(i, 2)
        at = lax.rem(i, per_stage)
        return pltpu.make_async_remote_copy(
            src_ref=x2.at[slot], dst_ref=obuf.at[at], send_sem=pp_send.at[slot], recv_sem=o_sem.at[at],
            device_id={"pp": i // per_stage}, device_id_type=MESH,
        )

    def hand_on(i):
        slot = lax.rem(i, 2)
        pl.when((i >= 2) & remote_out(i - 2))(lambda: next_copy(i).wait_send())
        sums = scatter_finish(i)
        own = rows_of(me, shard)
        for h in range(2):
            cols = pl.ds(h * half, half)
            m = sums[h].astype(BF16).astype(F32)
            x2[slot, :, cols] = (x1_own(i)[:, cols].astype(F32) + m + bdn_ref[:, cols]).astype(BF16)
        del own
        pl.when(stage < last)(lambda: next_copy(i).start())
        pl.when((stage == last) & (i < per_stage * last))(lambda: out_copy(i).start())

        @pl.when((stage == last) & (i >= per_stage * last))
        def _():
            obuf[lax.rem(i, per_stage)] = x2[slot]

    def x1_own(i):
        return x1.at[rows_of(me, shard)]

    def begin(i):
        x_arrival(i)
        gather_x(i).start()

    load_out.wait()
    pl.when(stage == 0)(lambda: begin(0))

    pl.when(lax.rem(stage, 2) == 1)(lambda: pl.semaphore_wait(turn_sem, 1))
    gather_w.start()
    gather_w.forward()
    gather_w.near()
    gather_w.far()
    pl.when(lax.rem(stage, 2) == 0)(
        lambda: pl.semaphore_signal(turn_sem, inc=1, device_id={"pp": stage + 1}, device_id_type=MESH)
    )
    load_qkv.wait()
    load_up.wait()
    load_dn.wait()

    pl.when(stage > 0)(lambda: begin(0))
    gather_x(0).forward()

    def step(i, carry):
        here = i < num_micro
        more = i < num_micro - 1
        pl.when(here)(lambda: attention_part(i))
        pl.when(here)(lambda: out_block(i, me, True))
        pl.when(i >= 1)(lambda: scatter_relay(i - 1))
        pl.when(i >= 1)(lambda: hand_on(i - 1))
        pl.when(here)(lambda: gather_c(i).forward())
        pl.when(more)(lambda: begin(i + 1))
        pl.when(here)(lambda: mlp_first(i))
        pl.when(more)(lambda: gather_x(i + 1).forward())
        pl.when(here)(lambda: mlp_second(i))
        return carry

    lax.fori_loop(0, num_micro + 1, step, 0)

    for i in range(num_micro - 2, num_micro):
        pl.when(stage < last)(lambda i=i: next_copy(i).wait_send())
        if i < per_stage * last:
            pl.when(stage == last)(lambda i=i: out_copy(i).wait_send())

    @pl.when(stage < last)
    def _():
        for j in range(per_stage):
            out_copy(j).wait_recv()

    out_ref[...] = obuf[...]


def solution(mesh):
    num_stages = mesh.shape["pp"]
    ring = mesh.shape["tp"]
    in_specs = (P("dp", None, "tp", None),
                P("pp", None), P("pp", None), P("pp", None, "tp"), P("pp", "tp"),
                P("pp", "tp", None, None), P("pp", None), P("pp", None), P("pp", None),
                P("pp", None, "tp"), P("pp", "tp"), P("pp", "tp", None), P("pp", None))
    out_specs = P(("dp", "pp"), None, "tp", None)

    def device_program(x_local, g1, s1, w_qkv, b_qkv, w_out, b_out, g2, s2, w_up, b_up, w_down, b_down):
        num_micro, batch, shard, width = x_local.shape
        local_heads, head_dim = w_out.shape[1], w_out.shape[2]
        own_k = local_heads * head_dim
        qkv_w, ff = w_qkv.shape[2], w_up.shape[2]
        rows = batch * shard
        seq = rows * ring
        half = width // 2
        per_stage = num_micro // num_stages
        hbm = pl.BlockSpec(memory_space=pl.ANY)
        vmem = pl.BlockSpec(memory_space=pltpu.VMEM)
        dma = pltpu.SemaphoreType.DMA
        out = pl.pallas_call(
            functools.partial(layer_kernel, num_stages, ring, head_dim),
            name="layers",
            out_shape=jax.ShapeDtypeStruct((per_stage, rows, width), BF16),
            in_specs=[hbm, vmem, vmem, hbm, vmem, hbm, vmem, vmem, vmem, hbm, vmem, hbm, vmem],
            out_specs=vmem,
            scratch_shapes=[
                pltpu.VMEM((width, qkv_w), BF16),
                pltpu.VMEM((own_k * ring, width), BF16),
                pltpu.VMEM((width, ff), BF16),
                pltpu.VMEM((ff, width), BF16),
                pltpu.VMEM((num_micro, rows, width), BF16),
                pltpu.VMEM((2, seq, width), BF16),
                pltpu.VMEM((seq, width), BF16),
                pltpu.VMEM((seq, qkv_w), BF16),
                pltpu.VMEM((2, ring, seq, own_k), BF16),
                pltpu.VMEM((seq, width), F32),
                pltpu.VMEM((seq, width), BF16),
                pltpu.VMEM((seq, ff), BF16),
                pltpu.VMEM((2, seq, width), BF16),
                pltpu.VMEM((2, 2, rows, half), BF16),
                pltpu.VMEM((2, 2, rows, half), BF16),
                pltpu.VMEM((2, 4, rows, half), BF16),
                pltpu.VMEM((2, rows, width), BF16),
                pltpu.VMEM((per_stage, rows, width), BF16),
                dma((4,)),
                dma((6,)),
                dma((6,)),
                dma((num_micro,)),
                dma((2, 6)),
                dma((2, 6)),
                dma((2, 6)),
                dma((2, 6)),
                dma((2, 6)),
                dma((2, 6)),
                dma((2,)),
                dma((per_stage,)),
                pltpu.SemaphoreType.REGULAR,
            ],
            compiler_params=pltpu.CompilerParams(
                collective_id=0, has_side_effects=True, vmem_limit_bytes=67_043_328
            ),
        )(
            x_local.reshape(num_micro, rows, width), g1, s1, w_qkv[0], b_qkv, w_out.reshape(own_k, width), b_out,
            g2, s2, w_up[0], b_up, w_down[0], b_down,
        )
        return out.reshape(per_stage, batch, shard, width)

    return jax.shard_map(device_program, mesh=mesh, in_specs=in_specs, out_specs=out_specs, check_vma=False)
```

```python
import functools

import jax
import jax.numpy as jnp
from jax import lax
from jax.experimental import pallas as pl
from jax.experimental.pallas import tpu as pltpu
from jax.sharding import PartitionSpec as P

LN_EPS = 1e-5
MESH = pl.DeviceIdType.MESH
F32 = jnp.float32
BF16 = jnp.bfloat16


def norm_rows(rows, gain, shift):
    rows = rows.astype(F32)
    centered = rows - jnp.mean(rows, axis=-1, keepdims=True)
    var = jnp.mean(centered * centered, axis=-1, keepdims=True)
    return (centered * lax.rsqrt(var + LN_EPS) * gain + shift).astype(BF16)


def layer_kernel(
    num_stages, ring, head_dim,
    x_hbm, g1_ref, s1_ref, wqkv_hbm, bqkv_ref, wout_hbm, bout_ref,
    g2_ref, s2_ref, wup_hbm, bup_ref, wdn_hbm, bdn_ref,
    out_ref,
    wqkv, wout, wup, wdn,
    xf, nb, qkv, cf, acc, x1, hid, part, fin, x2, obuf,
    w_sem, wg_send, wg_recv, xb_send, xr_send, xr_recv, ac_send, ac_recv,
    rs_send, rs_recv, pp_send, o_sem, turn_sem, free_sem,
):
    num_micro, shard, width = x_hbm.shape
    seq = shard * ring
    per_stage = num_micro // num_stages
    own_k = wout_hbm.shape[0]
    qkv_w = wqkv_hbm.shape[1]
    heads = own_k // head_dim
    half = width // 2
    last = num_stages - 1
    depth = xf.shape[0]

    me = lax.axis_index("tp")
    stage = lax.axis_index("pp")
    right = lax.rem(me + 1, ring)
    left = lax.rem(me + ring - 1, ring)
    opp = lax.rem(me + 2, ring)
    to_right, to_left, to_opp = {"tp": right}, {"tp": left}, {"tp": opp}

    def rows_of(owner, n):
        return pl.ds(pl.multiple_of(owner * n, n), n)

    def remote(src, dst, send, recv, device):
        return pltpu.make_async_remote_copy(
            src_ref=src, dst_ref=dst, send_sem=send, recv_sem=recv, device_id=device, device_id_type=MESH
        )

    def signal(sem, device):
        pl.semaphore_signal(sem, inc=1, device_id=device, device_id_type=MESH)

    barrier = pltpu.get_barrier_semaphore()

    def beside(pp):
        return ({"pp": pp}, {"tp": right, "pp": pp}, {"tp": left, "pp": pp})

    for device in (to_right, to_left, to_opp):
        signal(barrier, device)

    @pl.when(stage > 0)
    def _():
        for device in beside(stage - 1):
            signal(barrier, device)

    @pl.when(stage < last)
    def _():
        for device in beside(stage + 1):
            signal(barrier, device)

    pl.when(stage < last - 1)(lambda: signal(barrier, {"pp": last}))

    @pl.when(stage == last)
    def _():
        for q in range(last - 1):
            signal(barrier, {"pp": q})

    load_out = pltpu.make_async_copy(wout_hbm, wout.at[rows_of(me, own_k)], w_sem.at[0])
    load_qkv = pltpu.make_async_copy(wqkv_hbm, wqkv, w_sem.at[1])
    load_up = pltpu.make_async_copy(wup_hbm, wup, w_sem.at[2])
    load_dn = pltpu.make_async_copy(wdn_hbm, wdn, w_sem.at[3])
    load_out.start()
    load_qkv.start()
    load_up.start()
    load_dn.start()

    pl.semaphore_wait(
        barrier,
        3
        + jnp.where(stage > 0, 3, 0)
        + jnp.where(stage < last, 3, 0)
        + jnp.where(stage < last - 1, 1, 0)
        + jnp.where(stage == last, last - 1, 0),
    )

    class Gather:
        def __init__(self, piece, send, recv):
            self.piece, self.send, self.recv = piece, send, recv

        def copy(self, k, owner, h, device):
            return remote(self.piece(owner, h), self.piece(owner, h), self.send.at[k], self.recv.at[k], device)

        def hop1(self):
            return (
                self.copy(0, me, 0, to_right),
                self.copy(3, me, 1, to_left),
                self.copy(1, me, 1, to_right),
                self.copy(2, me, 0, to_left),
            )

        def fwd(self):
            return self.copy(4, left, 0, to_right), self.copy(5, right, 1, to_left)

        def start(self):
            for c in self.hop1():
                c.start()

        def recv_wait(self, k, owner, h):
            self.copy(k, owner, h, to_right).wait_recv()

        def forward(self):
            a, b = self.fwd()
            self.recv_wait(0, left, 0)
            a.start()
            self.recv_wait(3, right, 1)
            b.start()

        def near(self):
            self.recv_wait(1, left, 1)
            self.recv_wait(2, right, 0)

        def far(self):
            self.recv_wait(4, opp, 0)
            self.recv_wait(5, opp, 1)
            for c in self.fwd():
                c.wait_send()

        def sent(self):
            for c in self.hop1():
                c.wait_send()

    wk = own_k // 2
    gather_w = Gather(
        lambda owner, h: wout.at[pl.ds(pl.multiple_of(owner * own_k + h * wk, wk), wk)], wg_send, wg_recv
    )

    def gather_c(i):
        slot = lax.rem(i, 2)
        ch = seq // 2
        return Gather(lambda owner, h: cf.at[slot, owner, pl.ds(h * ch, ch)], ac_send.at[slot], ac_recv.at[slot])

    xh = shard // 2

    def gather_x(i):
        slot = lax.rem(i, depth)

        def piece(owner, h):
            return xf.at[slot, pl.ds(pl.multiple_of(owner * shard + h * xh, xh), xh)]

        return Gather(piece, xr_send.at[slot], xr_recv.at[slot])

    def x_own(i, src):
        slot = lax.rem(i, depth)
        return pltpu.make_async_copy(src, xf.at[slot, rows_of(me, shard)], xr_recv.at[slot, 6])

    def x_copies(i, src, send, pp):
        g = gather_x(i)

        def copy(k, h, tp):
            return remote(src(h), g.piece(me, h), send.at[k], g.recv.at[k], {"tp": tp, "pp": pp})

        return copy(0, 0, right), copy(3, 1, left), copy(1, 1, right), copy(2, 0, left)

    def begin_copies(i):
        return x_copies(i, lambda h: x_hbm.at[i, pl.ds(h * xh, xh)], xb_send.at[lax.rem(i, depth)], stage)

    def begin(i):
        for c in begin_copies(i):
            c.start()
        x_own(i, x_hbm.at[i]).start()

    def scatter(i, c):
        slot = lax.rem(i, 2)
        cols = pl.ds(c * half, half)

        def copy(k, owner, device):
            return remote(
                part.at[slot, rows_of(owner, shard), cols], fin.at[slot, k, :, cols],
                rs_send.at[slot, c, k], rs_recv.at[slot, c, k], device,
            )

        return copy(2, opp, to_opp), copy(0, right, to_right), copy(1, left, to_left)

    def ln_shard(i, owner):
        at = rows_of(owner, shard)
        nb[at] = norm_rows(xf[lax.rem(i, depth), at], g1_ref[...], s1_ref[...])

    causal = lax.broadcasted_iota(jnp.int32, (seq, seq), 0) >= lax.broadcasted_iota(jnp.int32, (seq, seq), 1)

    def attention_part(i):
        slot = lax.rem(i, 2)
        gx = gather_x(i)
        x_own(i, x_hbm.at[i]).wait()
        ln_shard(i, me)
        gx.near()
        ln_shard(i, left)
        ln_shard(i, right)
        gx.far()

        @pl.when(stage == 0)
        def _():
            for c in begin_copies(i):
                c.wait_send()

        ln_shard(i, opp)
        for lo, hi in ((0, 768), (768, 1536), (1536, qkv_w)):
            got = jnp.dot(nb[...], wqkv[:, lo:hi], preferred_element_type=F32)
            qkv[:, lo:hi] = (got + bqkv_ref[:, lo:hi]).astype(BF16)

        def part_of(n, j):
            at = (3 * n + j) * head_dim
            return qkv[:, at : at + head_dim]

        scores = [
            lax.dot_general(part_of(n, 0), part_of(n, 1), (((1,), (1,)), ((), ())), preferred_element_type=F32)
            for n in range(heads)
        ]
        probs = []
        for s in scores:
            s = jnp.where(causal, s * head_dim**-0.5, -1e30)
            e = jnp.exp(s - jnp.max(s, axis=-1, keepdims=True))
            probs.append((e * (1.0 / jnp.sum(e, axis=-1, keepdims=True))).astype(BF16))
        outs = [jnp.dot(p, part_of(n, 2), preferred_element_type=F32).astype(BF16) for n, p in enumerate(probs)]
        cf[slot, me] = jnp.concatenate(outs, axis=-1)
        gather_c(i).start()

    chunk = 512

    def out_block(i, owner, cols):
        return jnp.dot(cf[lax.rem(i, 2), owner], wout[rows_of(owner, own_k), cols], preferred_element_type=F32)

    def over_columns(f, lo=0, hi=width):
        for at in range(lo, hi, chunk):
            f(pl.ds(at, min(chunk, hi - at)))

    def out_own(i):
        def f(cols):
            acc[:, cols] = out_block(i, me, cols)

        over_columns(f)

    def mlp_first(i):
        slot = lax.rem(i, depth)
        gc = gather_c(i)
        gc.near()

        def near(cols):
            acc[:, cols] = acc[:, cols] + out_block(i, left, cols) + out_block(i, right, cols)

        over_columns(near)
        gc.far()

        def far(cols):
            a = (acc[:, cols] + out_block(i, opp, cols)).astype(BF16).astype(F32)
            x1[:, cols] = (xf[slot, :, cols].astype(F32) + a + bout_ref[:, cols]).astype(BF16)

        over_columns(far)
        gc.sent()

        @pl.when((stage > 0) & (i < num_micro - depth))
        def _():
            for k, device in zip((0, 2, 1), beside(stage - 1)):
                signal(free_sem.at[k], device)

        for r in range(ring):
            at = pl.ds(r * shard, shard)
            nb[at] = norm_rows(x1[at], g2_ref[...], s2_ref[...])

        def up(cols):
            got = jnp.dot(nb[...], wup[:, cols], preferred_element_type=F32) + bup_ref[:, cols]
            hid[:, cols] = jnp.maximum(got, 0.0).astype(BF16)

        over_columns(up)

    def mlp_second(i):
        slot = lax.rem(i, 2)

        def down(cols):
            part[slot, :, cols] = jnp.dot(hid[...], wdn[:, cols], preferred_element_type=F32).astype(BF16)

        for c in range(2):
            over_columns(down, c * half, (c + 1) * half)
            for copy in scatter(i, c):
                copy.start()

    def next_copies(i):
        slot = lax.rem(i, 2)
        send = pp_send.at[slot]
        pp = lax.rem(stage + 1, num_stages)
        own = remote(
            x2.at[slot], xf.at[lax.rem(i, depth), rows_of(me, shard)], send.at[4],
            xr_recv.at[lax.rem(i, depth), 6], {"pp": pp},
        )
        return *x_copies(i, lambda h: x2.at[slot, pl.ds(h * xh, xh)], send, pp), own

    def out_copy(i):
        slot = lax.rem(i, 2)
        at = lax.rem(i, per_stage)
        return remote(x2.at[slot], obuf.at[at], pp_send.at[slot, 4], o_sem.at[at], {"pp": i // per_stage})

    def sent_on(i):
        @pl.when(stage < last)
        def _():
            for c in next_copies(i):
                c.wait_send()

        pl.when((stage == last) & (i < per_stage * last))(lambda: out_copy(i).wait_send())

    def hand_on(i):
        slot = lax.rem(i, 2)
        pl.when(i >= 2)(lambda: sent_on(i - 2))
        own = rows_of(me, shard)
        for c in range(2):
            copies = scatter(i, c)
            for copy in copies:
                copy.wait_recv()
            cols = pl.ds(c * half, half)
            m = part[slot, own, cols].astype(F32)
            for k in range(3):
                m = m + fin[slot, k, :, cols].astype(F32)
            m = m.astype(BF16).astype(F32)
            x2[slot, :, cols] = (x1[own, cols].astype(F32) + m + bdn_ref[:, cols]).astype(BF16)

        @pl.when(stage < last)
        def _():
            @pl.when(i >= depth)
            def _():
                for k in range(3):
                    pl.semaphore_wait(free_sem.at[k], 1)

            for c in next_copies(i):
                c.start()

        pl.when((stage == last) & (i < per_stage * last))(lambda: out_copy(i).start())

        @pl.when((stage == last) & (i >= per_stage * last))
        def _():
            obuf[lax.rem(i, per_stage)] = x2[slot]

        for c in range(2):
            for copy in scatter(i, c):
                copy.wait_send()

    @pl.when(stage == 0)
    def _():
        begin(0)
        begin(1)

    load_out.wait()

    pl.when(lax.rem(stage, 2) == 1)(lambda: pl.semaphore_wait(turn_sem, 1))
    gather_w.start()
    gather_w.forward()
    gather_w.near()
    gather_w.far()
    gather_w.sent()
    pl.when(lax.rem(stage, 2) == 0)(lambda: signal(turn_sem, {"pp": stage + 1}))
    load_qkv.wait()
    load_up.wait()
    load_dn.wait()
    gather_x(0).forward()

    def step(i, carry):
        here = i < num_micro

        @pl.when(here)
        def _():
            attention_part(i)
            out_own(i)

        pl.when(i >= 1)(lambda: hand_on(i - 1))
        pl.when(here)(lambda: gather_c(i).forward())
        pl.when((stage == 0) & (i < num_micro - 2))(lambda: begin(i + 2))
        pl.when(here)(lambda: mlp_first(i))
        pl.when(i < num_micro - 1)(lambda: gather_x(i + 1).forward())
        pl.when(here)(lambda: mlp_second(i))
        return carry

    lax.fori_loop(0, num_micro + 1, step, 0)

    for i in range(num_micro - 2, num_micro):
        sent_on(i)

    @pl.when(stage < last)
    def _():
        for j in range(per_stage):
            out_copy(j).wait_recv()

    out_ref[...] = obuf[...]


def solution(mesh):
    num_stages = mesh.shape["pp"]
    ring = mesh.shape["tp"]
    in_specs = (P("dp", None, "tp", None),
                P("pp", None), P("pp", None), P("pp", None, "tp"), P("pp", "tp"),
                P("pp", "tp", None, None), P("pp", None), P("pp", None), P("pp", None),
                P("pp", None, "tp"), P("pp", "tp"), P("pp", "tp", None), P("pp", None))
    out_specs = P(("dp", "pp"), None, "tp", None)

    def device_program(x_local, g1, s1, w_qkv, b_qkv, w_out, b_out, g2, s2, w_up, b_up, w_down, b_down):
        num_micro, batch, shard, width = x_local.shape
        local_heads, head_dim = w_out.shape[1], w_out.shape[2]
        own_k = local_heads * head_dim
        qkv_w, ff = w_qkv.shape[2], w_up.shape[2]
        rows = batch * shard
        seq = rows * ring
        per_stage = num_micro // num_stages
        hbm = pl.BlockSpec(memory_space=pl.ANY)
        vmem = pl.BlockSpec(memory_space=pltpu.VMEM)
        dma = pltpu.SemaphoreType.DMA
        out = pl.pallas_call(
            functools.partial(layer_kernel, num_stages, ring, head_dim),
            name="layers",
            out_shape=jax.ShapeDtypeStruct((per_stage, rows, width), BF16),
            in_specs=[hbm, vmem, vmem, hbm, vmem, hbm, vmem, vmem, vmem, hbm, vmem, hbm, vmem],
            out_specs=vmem,
            scratch_shapes=[
                pltpu.VMEM((width, qkv_w), BF16),
                pltpu.VMEM((own_k * ring, width), BF16),
                pltpu.VMEM((width, ff), BF16),
                pltpu.VMEM((ff, width), BF16),
                pltpu.VMEM((4, seq, width), BF16),
                pltpu.VMEM((seq, width), BF16),
                pltpu.VMEM((seq, qkv_w), BF16),
                pltpu.VMEM((2, ring, seq, own_k), BF16),
                pltpu.VMEM((seq, width), F32),
                pltpu.VMEM((seq, width), BF16),
                pltpu.VMEM((seq, ff), BF16),
                pltpu.VMEM((2, seq, width), BF16),
                pltpu.VMEM((2, 3, rows, width), BF16),
                pltpu.VMEM((2, rows, width), BF16),
                pltpu.VMEM((per_stage, rows, width), BF16),
                dma((4,)),
                dma((6,)),
                dma((6,)),
                dma((4, 4)),
                dma((4, 6)),
                dma((4, 7)),
                dma((2, 6)),
                dma((2, 6)),
                dma((2, 2, 3)),
                dma((2, 2, 3)),
                dma((2, 5)),
                dma((per_stage,)),
                pltpu.SemaphoreType.REGULAR,
                pltpu.SemaphoreType.REGULAR((3,)),
            ],
            compiler_params=pltpu.CompilerParams(
                collective_id=0, has_side_effects=True, vmem_limit_bytes=67_043_328
            ),
        )(
            x_local.reshape(num_micro, rows, width), g1, s1, w_qkv[0], b_qkv, w_out.reshape(own_k, width), b_out,
            g2, s2, w_up[0], b_up, w_down[0], b_down,
        )
        return out.reshape(per_stage, batch, shard, width)

    return jax.shard_map(device_program, mesh=mesh, in_specs=in_specs, out_specs=out_specs, check_vma=False)
```

```python
import functools

import jax
import jax.numpy as jnp
from jax import lax
from jax.experimental import pallas as pl
from jax.experimental.pallas import tpu as pltpu
from jax.sharding import PartitionSpec as P

LN_EPS = 1e-5
MESH = pl.DeviceIdType.MESH
PARTS = 2
CUT_FIFTHS = (2, 2, 1)
POINTS = {"H0": 2, "He": 2, "Ho": 2, "F0": 5, "Fe": 5, "Fo": 6, "f0": 6, "fe": 6, "fo": 6}
F32 = jnp.float32
BF16 = jnp.bfloat16


def norm_rows(rows, gain, shift):
    rows = rows.astype(F32)
    centered = rows - jnp.mean(rows, axis=-1, keepdims=True)
    var = jnp.mean(centered * centered, axis=-1, keepdims=True)
    return (centered * lax.rsqrt(var + LN_EPS) * gain + shift).astype(BF16)


def layer_kernel(
    num_stages, ring, head_dim,
    x_hbm, g1_ref, s1_ref, wqkv_hbm, bqkv_ref, wout_hbm, bout_ref,
    g2_ref, s2_ref, wup_hbm, bup_ref, wdn_hbm, bdn_ref,
    out_ref,
    wqkv, wout, wup, wdn,
    xf, nb, qkv, cf, acc, x1, hid, part, fin, x2, obuf,
    w_sem, wg_send, wg_recv, wh_send, wh_recv, wx_send, wx_recv, wr_send, wr_recv, xb_send, xr_send, xr_recv, ac_send, ac_recv,
    rs_send, rs_recv, st_send, pp_send, o_sem, turn_sem, free_sem,
):
    num_micro, shard, width = x_hbm.shape
    seq = shard * ring
    per_stage = num_micro // num_stages
    own_k = wout_hbm.shape[0]
    qkv_w = wqkv_hbm.shape[1]
    heads = own_k // head_dim
    fifth = width // 5
    cuts = tuple(pl.ds(sum(CUT_FIFTHS[:c]) * fifth, n * fifth) for c, n in enumerate(CUT_FIFTHS))
    last = num_stages - 1
    depth = xf.shape[0]

    me = lax.axis_index("tp")
    stage = lax.axis_index("pp")
    right = lax.rem(me + 1, ring)
    left = lax.rem(me + ring - 1, ring)
    opp = lax.rem(me + 2, ring)
    to_right, to_left, to_opp = {"tp": right}, {"tp": left}, {"tp": opp}

    def rows_of(owner, n):
        return pl.ds(pl.multiple_of(owner * n, n), n)

    def remote(src, dst, send, recv, device):
        return pltpu.make_async_remote_copy(
            src_ref=src, dst_ref=dst, send_sem=send, recv_sem=recv, device_id=device, device_id_type=MESH
        )

    def signal(sem, device):
        pl.semaphore_signal(sem, inc=1, device_id=device, device_id_type=MESH)

    lends = (stage < 2) | (stage == 3)

    def helper(p):
        return stage + (jnp.where(stage == 3, 2, last - 1), 2)[p]

    def helped(p):
        return stage - (jnp.where(stage == 5, 2, last - 1), 2)[p]

    def helps(p):
        return ((stage >= last - 1) | (stage == 5), (stage == 2) | (stage == 3) | (stage == 5))[p]

    barrier = pltpu.get_barrier_semaphore()

    def beside(pp):
        return ({"pp": pp}, {"tp": right, "pp": pp}, {"tp": left, "pp": pp})

    for device in (to_right, to_left, to_opp):
        signal(barrier, device)

    @pl.when(stage > 0)
    def _():
        for device in beside(stage - 1):
            signal(barrier, device)

    @pl.when(stage < last)
    def _():
        for device in beside(stage + 1):
            signal(barrier, device)

    pl.when(stage < last - 1)(lambda: signal(barrier, {"pp": last}))

    for here, there in ((0, 1), (1, 0)):
        pl.when(stage == here)(lambda there=there: signal(barrier, {"tp": opp, "pp": there}))

    @pl.when(lends)
    def _():
        for p in range(2):
            signal(barrier, {"pp": helper(p)})

    pl.when(helps(0))(lambda: signal(barrier, {"pp": helped(0)}))
    pl.when(helps(1))(lambda: signal(barrier, {"pp": helped(1)}))

    @pl.when(stage == last)
    def _():
        for q in range(last - 1):
            signal(barrier, {"pp": q})

    load_out = pltpu.make_async_copy(wout_hbm, wout.at[rows_of(me, own_k)], w_sem.at[0])
    load_qkv = pltpu.make_async_copy(wqkv_hbm, wqkv, w_sem.at[1])
    load_up = pltpu.make_async_copy(wup_hbm, wup, w_sem.at[2])
    load_dn = pltpu.make_async_copy(wdn_hbm, wdn, w_sem.at[3])
    load_out.start()
    load_qkv.start()
    load_up.start()
    pl.when(~(helps(0) | helps(1)))(load_dn.start)

    pl.semaphore_wait(
        barrier,
        3
        + jnp.where(stage > 0, 3, 0)
        + jnp.where(stage < last, 3, 0)
        + jnp.where(stage < last - 1, 1, 0)
        + jnp.where(stage == last, last - 1, 0)
        + jnp.where(stage < 2, 1, 0)
        + jnp.where(lends, 2, 0)
        + jnp.where(helps(0), 1, 0)
        + jnp.where(helps(1), 1, 0),
    )

    class Gather:
        def __init__(self, piece, send, recv, parts=PARTS):
            self.piece, self.send, self.recv, self.parts = piece, send, recv, parts
            self.straight = None

        def copy(self, k, src, dst, device):
            return remote(src, dst, self.send.at[k], self.recv.at[k], device)

        def near_copies(self, src, right_device, left_device):
            n = self.parts
            first = []
            for j in range(n):
                first.append(self.copy(j, src(0, j), self.piece(me, 0, j), right_device))
                first.append(self.copy(n + j, src(1, j), self.piece(me, 1, j), left_device))
            return (
                *first,
                self.copy(2 * n, src(1, None), self.piece(me, 1, None), right_device),
                self.copy(2 * n + 1, src(0, None), self.piece(me, 0, None), left_device),
            )

        def hop1(self):
            return self.near_copies(lambda h, j: self.piece(me, h, j), to_right, to_left)

        def fwd(self):
            n = self.parts
            pairs = []
            for j in range(n):
                pairs.append((j, self.copy(2 * n + 2 + j, self.piece(left, 0, j), self.piece(left, 0, j), to_right)))
                pairs.append((n + j, self.copy(3 * n + 2 + j, self.piece(right, 1, j), self.piece(right, 1, j), to_left)))
            return pairs

        def start(self):
            for c in self.hop1():
                c.start()

        def arrived(self, k, owner, h, j):
            self.copy(k, self.piece(owner, h, j), self.piece(owner, h, j), to_right).wait_recv()

        def forward(self):
            n = self.parts
            for k, c in self.fwd():
                self.arrived(k, *((left, 0, k) if k < n else (right, 1, k - n)))
                c.start() if self.straight is None else pl.when(~self.straight)(c.start)

        def near(self):
            n = self.parts
            self.arrived(2 * n, left, 1, None)
            self.arrived(2 * n + 1, right, 0, None)

        def far(self):
            n = self.parts
            for j in range(n):
                self.arrived(2 * n + 2 + j, opp, 0, j)
                self.arrived(3 * n + 2 + j, opp, 1, j)

            def forwarded():
                for _, c in self.fwd():
                    c.wait_send()

            forwarded() if self.straight is None else pl.when(~self.straight)(forwarded)

        def sent(self):
            for c in self.hop1():
                c.wait_send()

        def finish(self):
            self.near()
            self.far()
            self.sent()

    class Whole:
        def __init__(self, by_y, by_x):
            self.by_y, self.by_x = by_y, by_x
            self.first = Gather(self.piece(0, by_y), wg_send.at[0], wg_recv.at[0], 1)
            self.rest = Gather(self.piece(by_y, 2 * by_x), wg_send.at[1], wg_recv.at[1], 1)

        @staticmethod
        def half_of(n, h):
            first = -(-n // 32) * 16
            return (0, first) if h == 0 else (first, n - first)

        def piece(self, lo, n):
            def of(owner, h, j=None):
                at, size = self.half_of(n, h)
                return wout.at[pl.ds(pl.multiple_of(owner * own_k + lo + at, 16), size)]

            return of

        def path(self, p):
            return self.piece(self.by_y + p * self.by_x, self.by_x)

        def lent(self, p):
            def of(owner, h, j=None):
                at, size = self.half_of(self.by_x, h)
                return wdn.at[pl.ds(pl.multiple_of((p * ring + owner) * self.by_x + at, 16), size)]

            return of

        def lend(self, p, h, pp):
            return remote(self.path(p)(me, h), self.lent(p)(me, h), wx_send.at[p, h], wx_recv.at[p, h], {"pp": pp})

        def give_back(self, p, k, pp):
            owner, h = others[k]
            return remote(
                self.lent(p)(owner, h), self.path(p)(owner, h), wr_send.at[p, k], wr_recv.at[p, k], {"pp": pp}
            )

        def helper_ring(self, p):
            return Gather(self.lent(p), wh_send.at[p], wh_recv.at[p], 1)

        def help_gather(self, p, now):
            pp, g = helped(p), self.helper_ring(p)
            for h in range(2):
                self.lend(p, h, pp).wait_recv()
                for c in (g.hop1()[0], g.hop1()[3]) if h == 0 else (g.hop1()[1], g.hop1()[2]):
                    c.start()
            for k in range(6):
                g.arrived(k, *others[k], None)
                if k < 2:
                    g.fwd()[k][1].start()
                if now:
                    self.give_back(p, k, pp).start()
            if not now:
                pl.semaphore_wait(turn_sem.at[2], 1)
                for k in range(6):
                    self.give_back(p, k, pp).start()

        def help_end(self, p):
            g = self.helper_ring(p)
            g.sent()
            for _, c in g.fwd():
                c.wait_send()
            for k in range(6):
                self.give_back(p, k, helped(p)).wait_send()

        def lend_all(self):
            for h in range(2):
                for p in range(2):
                    self.lend(p, h, helper(p)).start()

        def lent_all(self):
            for h in range(2):
                for p in range(2):
                    self.lend(p, h, helper(p)).wait_send()

        def end(self):
            self.first.finish()
            pl.when(stage == 0)(lambda: signal(turn_sem.at[0], {"pp": stage + 1}))
            for p in range(2):
                for k in range(6):
                    self.give_back(p, k, helper(p)).wait_recv()

    others = ((left, 0), (right, 1), (left, 1), (right, 0), (opp, 0), (opp, 1))
    whole_even = Whole(own_k // 2, own_k // 4)
    whole_odd = Whole(own_k // 2, own_k // 4)

    def gather_c(i):
        slot = lax.rem(i, 2)
        ch = seq // 2
        cn = ch // PARTS

        def piece(owner, h, j=None):
            rows = pl.ds(h * ch, ch) if j is None else pl.ds(h * ch + j * cn, cn)
            return cf.at[slot, owner, rows]

        return Gather(piece, ac_send.at[slot], ac_recv.at[slot])

    xh = shard // 2

    xn = width // PARTS

    def x_part(ref, h, j):
        at = pl.ds(h * xh, xh)
        return ref.at[at] if j is None else ref.at[at, pl.ds(j * xn, xn)]

    def gather_x(i):
        slot = lax.rem(i, depth)

        def piece(owner, h, j=None):
            at = pl.ds(pl.multiple_of(owner * shard + h * xh, xh), xh)
            return xf.at[slot, at] if j is None else xf.at[slot, at, pl.ds(j * xn, xn)]

        g = Gather(piece, xr_send.at[slot], xr_recv.at[slot])
        g.straight = (stage == 1) & (i == 0)
        return g

    def x_own(i, src):
        slot = lax.rem(i, depth)
        return pltpu.make_async_copy(src, xf.at[slot, rows_of(me, shard)], xr_recv.at[slot, 4 * PARTS + 2])

    def x_copies(i, ref, send, pp):
        g = gather_x(i)
        g.send = send
        return g.near_copies(lambda h, j: x_part(ref, h, j), {"tp": right, "pp": pp}, {"tp": left, "pp": pp})

    def straight_copies():
        g = gather_x(0)
        n = g.parts
        pp = {"tp": opp, "pp": lax.rem(stage + 1, num_stages)}
        return [
            remote(x_part(x2.at[0], h, j), g.piece(me, h, j), st_send.at[h * n + j], g.recv.at[(2 + h) * n + 2 + j], pp)
            for j in range(n)
            for h in range(2)
        ]

    def begin_copies(i):
        return x_copies(i, x_hbm.at[i], xb_send.at[lax.rem(i, depth)], stage)

    def begin(i):
        for c in begin_copies(i):
            c.start()
        x_own(i, x_hbm.at[i]).start()

    def scatter(i, c):
        slot = lax.rem(i, 2)
        cols = cuts[c]

        def copy(k, owner, device):
            return remote(
                part.at[slot, rows_of(owner, shard), cols], fin.at[slot, k, :, cols],
                rs_send.at[slot, c, k], rs_recv.at[slot, c, k], device,
            )

        return copy(2, opp, to_opp), copy(0, right, to_right), copy(1, left, to_left)

    def ln_shard(i, owner):
        at = rows_of(owner, shard)
        nb[at] = norm_rows(xf[lax.rem(i, depth), at], g1_ref[...], s1_ref[...])

    causal = lax.broadcasted_iota(jnp.int32, (seq, seq), 0) >= lax.broadcasted_iota(jnp.int32, (seq, seq), 1)

    def slot_at(s, i):
        even = lax.rem(stage, 2) == 0
        kinds = {"0": stage == 0, "e": even & (stage > 0), "o": ~even}

        def any_of(letter):
            found = [kinds[k] for k in kinds if POINTS[letter + k] == s]
            return functools.reduce(jnp.logical_or, found) if found else None

        h, f, f_first = any_of("H"), any_of("F"), any_of("f")
        if h is not None:
            pl.when(h & (i >= 1))(lambda: hand_on(i - 1))
        go = None
        if f is not None:
            go = f & (i > 0)
        if f_first is not None:
            g = f_first & (i == 0)
            go = g if go is None else go | g
        if go is not None:
            pl.when(go & (i < num_micro - 1))(lambda: gather_x(i + 1).forward())
        if s == 3:
            pl.when((stage == 0) & (i < num_micro - 2))(lambda: begin(i + 2))

    def attention_part(i):
        slot = lax.rem(i, 2)
        gx = gather_x(i)
        x_own(i, x_hbm.at[i]).wait()
        ln_shard(i, me)
        gx.near()
        ln_shard(i, left)
        ln_shard(i, right)
        gx.far()

        @pl.when(stage == 0)
        def _():
            for c in begin_copies(i):
                c.wait_send()

        ln_shard(i, opp)
        for lo, hi in ((0, 768), (768, 1536), (1536, qkv_w)):
            got = jnp.dot(nb[...], wqkv[:, lo:hi], preferred_element_type=F32)
            qkv[:, lo:hi] = (got + bqkv_ref[:, lo:hi]).astype(BF16)
        slot_at(1, i)

        def part_of(n, j):
            at = (3 * n + j) * head_dim
            return qkv[:, at : at + head_dim]

        scores = [
            lax.dot_general(part_of(n, 0), part_of(n, 1), (((1,), (1,)), ((), ())), preferred_element_type=F32)
            for n in range(heads)
        ]
        probs = []
        for s in scores:
            s = jnp.where(causal, s * head_dim**-0.5, -1e30)
            e = jnp.exp(s - jnp.max(s, axis=-1, keepdims=True))
            probs.append((e * (1.0 / jnp.sum(e, axis=-1, keepdims=True))).astype(BF16))
        outs = [jnp.dot(p, part_of(n, 2), preferred_element_type=F32).astype(BF16) for n, p in enumerate(probs)]
        cf[slot, me] = jnp.concatenate(outs, axis=-1)
        gather_c(i).start()

    chunk = 512

    def out_block(i, owner, cols):
        return jnp.dot(cf[lax.rem(i, 2), owner], wout[rows_of(owner, own_k), cols], preferred_element_type=F32)

    def over_columns(f, lo=0, hi=width):
        for at in range(lo, hi, chunk):
            f(pl.ds(at, min(chunk, hi - at)))

    def out_own(i):
        def f(cols):
            acc[:, cols] = out_block(i, me, cols)

        over_columns(f)

    def mlp_first(i):
        slot = lax.rem(i, depth)
        gc = gather_c(i)
        pl.when((stage == 0) & (i == 0))(whole_even.end)
        pl.when((stage == 1) & (i == 0))(whole_odd.end)
        gc.near()

        def near(cols):
            acc[:, cols] = acc[:, cols] + out_block(i, left, cols) + out_block(i, right, cols)

        over_columns(near)
        slot_at(4, i)
        gc.far()

        def far(cols):
            a = (acc[:, cols] + out_block(i, opp, cols)).astype(BF16).astype(F32)
            x1[:, cols] = (xf[slot, :, cols].astype(F32) + a + bout_ref[:, cols]).astype(BF16)

        over_columns(far)
        gc.sent()
        slot_at(5, i)

        @pl.when((stage > 0) & (i < num_micro - depth))
        def _():
            for k, device in zip((0, 2, 1), beside(stage - 1)):
                signal(free_sem.at[k], device)

        for r in range(ring):
            at = pl.ds(r * shard, shard)
            nb[at] = norm_rows(x1[at], g2_ref[...], s2_ref[...])

        def up(cols):
            got = jnp.dot(nb[...], wup[:, cols], preferred_element_type=F32) + bup_ref[:, cols]
            hid[:, cols] = jnp.maximum(got, 0.0).astype(BF16)

        over_columns(up)

    def mlp_second(i):
        slot = lax.rem(i, 2)

        def down(cols):
            part[slot, :, cols] = jnp.dot(hid[...], wdn[:, cols], preferred_element_type=F32).astype(BF16)

        for c in range(len(cuts)):
            over_columns(down, cuts[c].start, cuts[c].start + cuts[c].size)
            for copy in scatter(i, c):
                copy.start()
            if c == 0:
                slot_at(7, i)

    def next_copies(i):
        slot = lax.rem(i, 2)
        send = pp_send.at[slot]
        pp = lax.rem(stage + 1, num_stages)
        own = remote(
            x2.at[slot], xf.at[lax.rem(i, depth), rows_of(me, shard)], send.at[2 * PARTS + 2],
            xr_recv.at[lax.rem(i, depth), 4 * PARTS + 2], {"pp": pp},
        )
        return *x_copies(i, x2.at[slot], send, pp), own

    def out_copy(i):
        slot = lax.rem(i, 2)
        at = lax.rem(i, per_stage)
        return remote(x2.at[slot], obuf.at[at], pp_send.at[slot, 2 * PARTS + 2], o_sem.at[at], {"pp": i // per_stage})

    def sent_on(i):
        @pl.when(stage < last)
        def _():
            for c in next_copies(i):
                c.wait_send()

            @pl.when((stage == 0) & (i == 0))
            def _():
                for c in straight_copies():
                    c.wait_send()

        pl.when((stage == last) & (i < per_stage * last))(lambda: out_copy(i).wait_send())

    def hand_on(i):
        slot = lax.rem(i, 2)
        pl.when(i >= 2)(lambda: sent_on(i - 2))
        own = rows_of(me, shard)
        for c in range(len(cuts)):
            copies = scatter(i, c)
            for copy in copies:
                copy.wait_recv()
            cols = cuts[c]
            m = part[slot, own, cols].astype(F32)
            for k in range(3):
                m = m + fin[slot, k, :, cols].astype(F32)
            m = m.astype(BF16).astype(F32)
            x2[slot, :, cols] = (x1[own, cols].astype(F32) + m + bdn_ref[:, cols]).astype(BF16)

        @pl.when(stage < last)
        def _():
            @pl.when(i >= depth)
            def _():
                for k in range(3):
                    pl.semaphore_wait(free_sem.at[k], 1)

            @pl.when((stage == 0) & (i == 0))
            def _():
                for c in straight_copies():
                    c.start()

            for c in next_copies(i):
                c.start()

        pl.when((stage == last) & (i < per_stage * last))(lambda: out_copy(i).start())

        @pl.when((stage == last) & (i >= per_stage * last))
        def _():
            obuf[lax.rem(i, per_stage)] = x2[slot]

        for c in range(len(cuts)):
            for copy in scatter(i, c):
                copy.wait_send()

    load_out.wait()
    even = lax.rem(stage, 2) == 0

    @pl.when(stage == 0)
    def _():
        begin(0)
        whole_even.lend_all()
        gather_x(0).forward()
        whole_even.first.start()
        begin(1)
        whole_even.lent_all()
        signal(turn_sem.at[1], {"pp": stage + 1})

    @pl.when(stage == 1)
    def _():
        pl.semaphore_wait(turn_sem.at[1], 1)
        whole_odd.lend_all()
        pl.semaphore_wait(turn_sem.at[0], 1)
        whole_odd.first.start()
        whole_odd.first.forward()
        whole_odd.lent_all()

    @pl.when((stage > 1) & even)
    def _():
        w = whole_even
        for p in range(2):
            pl.when(helps(p))(lambda p=p: w.help_gather(p, True))
        for g in (w.first, w.rest):
            g.start()

        @pl.when(helps(0) | helps(1))
        def _():
            for p in range(2):
                pl.when(helps(p))(lambda p=p: w.help_end(p))
            load_dn.start()
            signal(turn_sem.at[2], {"pp": stage + 1})

        for g in (w.first, w.rest):
            g.forward()
        for g in (w.first, w.rest):
            g.finish()
        signal(turn_sem.at[0], {"pp": stage + 1})

    @pl.when((stage > 1) & ~even)
    def _():
        w = whole_odd
        pl.when(stage == 3)(w.lend_all)
        pl.when(stage == 3)(lambda: w.help_gather(1, False))
        pl.when(stage == last)(lambda: w.help_gather(0, False))

        @pl.when(stage == 5)
        def _():
            for p in range(2):
                w.help_gather(p, True)

        pl.semaphore_wait(turn_sem.at[0], 1)
        w.first.start()
        pl.when(stage != 3)(w.rest.start)
        for p in range(2):
            pl.when(helps(p))(lambda p=p: w.help_end(p))
        load_dn.start()
        w.first.forward()

        @pl.when(stage != 3)
        def _():
            w.rest.forward()
            w.first.finish()
            w.rest.finish()

        @pl.when(stage == 3)
        def _():
            w.lent_all()
            w.end()

    load_qkv.wait()
    load_up.wait()
    load_dn.wait()
    pl.when(stage > 0)(lambda: gather_x(0).forward())

    def step(i, carry):
        here = i < num_micro

        @pl.when(here)
        def _():
            slot_at(0, i)
            attention_part(i)
            out_own(i)

            @pl.when((stage == 0) & (i == 0))
            def _():
                whole_even.first.forward()

            slot_at(2, i)

        pl.when(i == num_micro)(lambda: hand_on(i - 1))

        @pl.when(here)
        def _():
            gather_c(i).forward()
            slot_at(3, i)
            mlp_first(i)
            slot_at(6, i)
            mlp_second(i)
            slot_at(8, i)

        return carry

    lax.fori_loop(0, num_micro + 1, step, 0)

    for i in range(num_micro - 2, num_micro):
        sent_on(i)

    @pl.when(stage < last)
    def _():
        for j in range(per_stage):
            out_copy(j).wait_recv()

    out_ref[...] = obuf[...]


def solution(mesh):
    num_stages = mesh.shape["pp"]
    ring = mesh.shape["tp"]
    in_specs = (P("dp", None, "tp", None),
                P("pp", None), P("pp", None), P("pp", None, "tp"), P("pp", "tp"),
                P("pp", "tp", None, None), P("pp", None), P("pp", None), P("pp", None),
                P("pp", None, "tp"), P("pp", "tp"), P("pp", "tp", None), P("pp", None))
    out_specs = P(("dp", "pp"), None, "tp", None)

    def device_program(x_local, g1, s1, w_qkv, b_qkv, w_out, b_out, g2, s2, w_up, b_up, w_down, b_down):
        num_micro, batch, shard, width = x_local.shape
        local_heads, head_dim = w_out.shape[1], w_out.shape[2]
        own_k = local_heads * head_dim
        qkv_w, ff = w_qkv.shape[2], w_up.shape[2]
        rows = batch * shard
        seq = rows * ring
        per_stage = num_micro // num_stages
        hbm = pl.BlockSpec(memory_space=pl.ANY)
        vmem = pl.BlockSpec(memory_space=pltpu.VMEM)
        dma = pltpu.SemaphoreType.DMA
        out = pl.pallas_call(
            functools.partial(layer_kernel, num_stages, ring, head_dim),
            name="layers",
            out_shape=jax.ShapeDtypeStruct((per_stage, rows, width), BF16),
            in_specs=[hbm, vmem, vmem, hbm, vmem, hbm, vmem, vmem, vmem, hbm, vmem, hbm, vmem],
            out_specs=vmem,
            scratch_shapes=[
                pltpu.VMEM((width, qkv_w), BF16),
                pltpu.VMEM((own_k * ring, width), BF16),
                pltpu.VMEM((width, ff), BF16),
                pltpu.VMEM((ff, width), BF16),
                pltpu.VMEM((4, seq, width), BF16),
                pltpu.VMEM((seq, width), BF16),
                pltpu.VMEM((seq, qkv_w), BF16),
                pltpu.VMEM((2, ring, seq, own_k), BF16),
                pltpu.VMEM((seq, width), F32),
                pltpu.VMEM((seq, width), BF16),
                pltpu.VMEM((seq, ff), BF16),
                pltpu.VMEM((2, seq, width), BF16),
                pltpu.VMEM((2, 3, rows, width), BF16),
                pltpu.VMEM((2, rows, width), BF16),
                pltpu.VMEM((per_stage, rows, width), BF16),
                dma((4,)),
                dma((2, 6)),
                dma((2, 6)),
                dma((2, 6)),
                dma((2, 6)),
                dma((2, 2)),
                dma((2, 2)),
                dma((2, 6)),
                dma((2, 6)),
                dma((4, 2 * PARTS + 2)),
                dma((4, 4 * PARTS + 2)),
                dma((4, 4 * PARTS + 3)),
                dma((2, 4 * PARTS + 2)),
                dma((2, 4 * PARTS + 2)),
                dma((2, len(CUT_FIFTHS), 3)),
                dma((2, len(CUT_FIFTHS), 3)),
                dma((2 * PARTS,)),
                dma((2, 2 * PARTS + 3)),
                dma((per_stage,)),
                pltpu.SemaphoreType.REGULAR((3,)),
                pltpu.SemaphoreType.REGULAR((3,)),
            ],
            compiler_params=pltpu.CompilerParams(
                collective_id=0, has_side_effects=True, vmem_limit_bytes=67_043_328
            ),
        )(
            x_local.reshape(num_micro, rows, width), g1, s1, w_qkv[0], b_qkv, w_out.reshape(own_k, width), b_out,
            g2, s2, w_up[0], b_up, w_down[0], b_down,
        )
        return out.reshape(per_stage, batch, shard, width)

    return jax.shard_map(device_program, mesh=mesh, in_specs=in_specs, out_specs=out_specs, check_vma=False)
```

```python
import functools

import jax
import jax.numpy as jnp
from jax import lax
from jax.experimental import pallas as pl
from jax.experimental.pallas import tpu as pltpu
from jax.sharding import PartitionSpec as P

LN_EPS = 1e-5
MESH = pl.DeviceIdType.MESH
PARTS = 2
CUT_FIFTHS = (2, 1, 2)
POINTS = {"H0": 2, "He": 2, "Ho": 2, "F0": 6, "Fe": 5, "Fo": 6, "f0": 6, "fe": 6, "fo": 6}
F32 = jnp.float32
BF16 = jnp.bfloat16


def norm_rows(rows, gain, shift):
    rows = rows.astype(F32)
    centered = rows - jnp.mean(rows, axis=-1, keepdims=True)
    var = jnp.mean(centered * centered, axis=-1, keepdims=True)
    return (centered * lax.rsqrt(var + LN_EPS) * gain + shift).astype(BF16)


def layer_kernel(
    num_stages, ring, head_dim,
    x_hbm, g1_ref, s1_ref, wqkv_hbm, bqkv_ref, wout_hbm, bout_ref,
    g2_ref, s2_ref, wup_hbm, bup_ref, wdn_hbm, bdn_ref,
    out_ref,
    wqkv, wout, wup, wdn,
    xf, nb, qkv, cf, acc, x1, hid, part, fin, x2, obuf,
    w_sem, wg_send, wg_recv, wh_send, wh_recv, wx_send, wx_recv, wr_send, wr_recv, xb_send, xr_send, xr_recv, ac_send, ac_recv,
    rs_send, rs_recv, st_send, pp_send, o_sem, turn_sem, free_sem,
):
    num_micro, shard, width = x_hbm.shape
    seq = shard * ring
    per_stage = num_micro // num_stages
    own_k = wout_hbm.shape[0]
    qkv_w = wqkv_hbm.shape[1]
    heads = own_k // head_dim
    fifth = width // 5
    cuts = tuple(pl.ds(sum(CUT_FIFTHS[:c]) * fifth, n * fifth) for c, n in enumerate(CUT_FIFTHS))
    last = num_stages - 1
    depth = xf.shape[0]

    me = lax.axis_index("tp")
    stage = lax.axis_index("pp")
    right = lax.rem(me + 1, ring)
    left = lax.rem(me + ring - 1, ring)
    opp = lax.rem(me + 2, ring)
    to_right, to_left, to_opp = {"tp": right}, {"tp": left}, {"tp": opp}

    def rows_of(owner, n):
        return pl.ds(pl.multiple_of(owner * n, n), n)

    def remote(src, dst, send, recv, device):
        return pltpu.make_async_remote_copy(
            src_ref=src, dst_ref=dst, send_sem=send, recv_sem=recv, device_id=device, device_id_type=MESH
        )

    def signal(sem, device):
        pl.semaphore_signal(sem, inc=1, device_id=device, device_id_type=MESH)

    lends = (stage < 2) | (stage == 3)

    def helper(p):
        return stage + (jnp.where(stage == 3, 2, last - 1), 2)[p]

    def helped(p):
        return stage - (jnp.where(stage == 5, 2, last - 1), 2)[p]

    def helps(p):
        return ((stage >= last - 1) | (stage == 5), (stage == 2) | (stage == 3) | (stage == 5))[p]

    barrier = pltpu.get_barrier_semaphore()

    def beside(pp):
        return ({"pp": pp}, {"tp": right, "pp": pp}, {"tp": left, "pp": pp})

    for device in (to_right, to_left, to_opp):
        signal(barrier, device)

    @pl.when(stage > 0)
    def _():
        for device in beside(stage - 1):
            signal(barrier, device)

    @pl.when(stage < last)
    def _():
        for device in beside(stage + 1):
            signal(barrier, device)

    pl.when(stage < last - 1)(lambda: signal(barrier, {"pp": last}))

    for here, there in ((0, 1), (1, 0)):
        pl.when(stage == here)(lambda there=there: signal(barrier, {"tp": opp, "pp": there}))

    @pl.when(lends)
    def _():
        for p in range(2):
            signal(barrier, {"pp": helper(p)})

    pl.when(helps(0))(lambda: signal(barrier, {"pp": helped(0)}))
    pl.when(helps(1))(lambda: signal(barrier, {"pp": helped(1)}))

    @pl.when(stage == last)
    def _():
        for q in range(last - 1):
            signal(barrier, {"pp": q})

    load_out = pltpu.make_async_copy(wout_hbm, wout.at[rows_of(me, own_k)], w_sem.at[0])
    load_qkv = pltpu.make_async_copy(wqkv_hbm, wqkv, w_sem.at[1])
    load_up = pltpu.make_async_copy(wup_hbm, wup, w_sem.at[2])
    load_dn = pltpu.make_async_copy(wdn_hbm, wdn, w_sem.at[3])
    load_out.start()
    load_qkv.start()
    load_up.start()
    pl.when(~(helps(0) | helps(1)))(load_dn.start)

    pl.semaphore_wait(
        barrier,
        3
        + jnp.where(stage > 0, 3, 0)
        + jnp.where(stage < last, 3, 0)
        + jnp.where(stage < last - 1, 1, 0)
        + jnp.where(stage == last, last - 1, 0)
        + jnp.where(stage < 2, 1, 0)
        + jnp.where(lends, 2, 0)
        + jnp.where(helps(0), 1, 0)
        + jnp.where(helps(1), 1, 0),
    )

    class Gather:
        def __init__(self, piece, send, recv, parts=PARTS):
            self.piece, self.send, self.recv, self.parts = piece, send, recv, parts
            self.straight = None

        def copy(self, k, src, dst, device):
            return remote(src, dst, self.send.at[k], self.recv.at[k], device)

        def near_copies(self, src, right_device, left_device):
            n = self.parts
            first = []
            for j in range(n):
                first.append(self.copy(j, src(0, j), self.piece(me, 0, j), right_device))
                first.append(self.copy(n + j, src(1, j), self.piece(me, 1, j), left_device))
            return (
                *first,
                self.copy(2 * n, src(1, None), self.piece(me, 1, None), right_device),
                self.copy(2 * n + 1, src(0, None), self.piece(me, 0, None), left_device),
            )

        def hop1(self):
            return self.near_copies(lambda h, j: self.piece(me, h, j), to_right, to_left)

        def fwd(self):
            n = self.parts
            pairs = []
            for j in range(n):
                pairs.append((j, self.copy(2 * n + 2 + j, self.piece(left, 0, j), self.piece(left, 0, j), to_right)))
                pairs.append((n + j, self.copy(3 * n + 2 + j, self.piece(right, 1, j), self.piece(right, 1, j), to_left)))
            return pairs

        def start(self):
            for c in self.hop1():
                c.start()

        def arrived(self, k, owner, h, j):
            self.copy(k, self.piece(owner, h, j), self.piece(owner, h, j), to_right).wait_recv()

        def forward(self):
            n = self.parts
            for k, c in self.fwd():
                self.arrived(k, *((left, 0, k) if k < n else (right, 1, k - n)))
                c.start() if self.straight is None else pl.when(~self.straight)(c.start)

        def near(self):
            n = self.parts
            self.arrived(2 * n, left, 1, None)
            self.arrived(2 * n + 1, right, 0, None)

        def far(self):
            n = self.parts
            for j in range(n):
                self.arrived(2 * n + 2 + j, opp, 0, j)
                self.arrived(3 * n + 2 + j, opp, 1, j)

            def forwarded():
                for _, c in self.fwd():
                    c.wait_send()

            forwarded() if self.straight is None else pl.when(~self.straight)(forwarded)

        def sent(self):
            for c in self.hop1():
                c.wait_send()

        def finish(self):
            self.near()
            self.far()
            self.sent()

    class Whole:
        def __init__(self, by_y, by_x):
            self.by_y, self.by_x = by_y, by_x
            self.first = Gather(self.piece(0, by_y), wg_send.at[0], wg_recv.at[0], 1)
            self.rest = Gather(self.piece(by_y, 2 * by_x), wg_send.at[1], wg_recv.at[1], 1)

        @staticmethod
        def half_of(n, h):
            first = -(-n // 32) * 16
            return (0, first) if h == 0 else (first, n - first)

        def piece(self, lo, n):
            def of(owner, h, j=None):
                at, size = self.half_of(n, h)
                return wout.at[pl.ds(pl.multiple_of(owner * own_k + lo + at, 16), size)]

            return of

        def path(self, p):
            return self.piece(self.by_y + p * self.by_x, self.by_x)

        def lent(self, p):
            def of(owner, h, j=None):
                at, size = self.half_of(self.by_x, h)
                return wdn.at[pl.ds(pl.multiple_of((p * ring + owner) * self.by_x + at, 16), size)]

            return of

        def lend(self, p, h, pp):
            return remote(self.path(p)(me, h), self.lent(p)(me, h), wx_send.at[p, h], wx_recv.at[p, h], {"pp": pp})

        def give_back(self, p, k, pp):
            owner, h = others[k]
            return remote(
                self.lent(p)(owner, h), self.path(p)(owner, h), wr_send.at[p, k], wr_recv.at[p, k], {"pp": pp}
            )

        def helper_ring(self, p):
            return Gather(self.lent(p), wh_send.at[p], wh_recv.at[p], 1)

        def help_gather(self, p, now):
            pp, g = helped(p), self.helper_ring(p)
            for h in range(2):
                self.lend(p, h, pp).wait_recv()
                for c in (g.hop1()[0], g.hop1()[3]) if h == 0 else (g.hop1()[1], g.hop1()[2]):
                    c.start()
            for k in range(6):
                g.arrived(k, *others[k], None)
                if k < 2:
                    g.fwd()[k][1].start()
                if now:
                    self.give_back(p, k, pp).start()
            if not now:
                pl.semaphore_wait(turn_sem.at[2], 1)
                for k in range(6):
                    self.give_back(p, k, pp).start()

        def help_end(self, p):
            g = self.helper_ring(p)
            g.sent()
            for _, c in g.fwd():
                c.wait_send()
            for k in range(6):
                self.give_back(p, k, helped(p)).wait_send()

        def lend_all(self):
            for h in range(2):
                for p in range(2):
                    self.lend(p, h, helper(p)).start()

        def lent_all(self):
            for h in range(2):
                for p in range(2):
                    self.lend(p, h, helper(p)).wait_send()

        def end(self):
            self.first.finish()
            pl.when(stage == 0)(lambda: signal(turn_sem.at[0], {"pp": stage + 1}))
            for p in range(2):
                for k in range(6):
                    self.give_back(p, k, helper(p)).wait_recv()

    others = ((left, 0), (right, 1), (left, 1), (right, 0), (opp, 0), (opp, 1))
    whole_even = Whole(own_k // 2, own_k // 4)
    whole_odd = Whole(9 * own_k // 20, 11 * own_k // 40)

    def gather_c(i):
        slot = lax.rem(i, 2)
        ch = seq // 2
        cn = ch // PARTS

        def piece(owner, h, j=None):
            rows = pl.ds(h * ch, ch) if j is None else pl.ds(h * ch + j * cn, cn)
            return cf.at[slot, owner, rows]

        return Gather(piece, ac_send.at[slot], ac_recv.at[slot])

    xh = shard // 2

    xn = width // PARTS

    def x_part(ref, h, j):
        at = pl.ds(h * xh, xh)
        return ref.at[at] if j is None else ref.at[at, pl.ds(j * xn, xn)]

    def gather_x(i):
        slot = lax.rem(i, depth)

        def piece(owner, h, j=None):
            at = pl.ds(pl.multiple_of(owner * shard + h * xh, xh), xh)
            return xf.at[slot, at] if j is None else xf.at[slot, at, pl.ds(j * xn, xn)]

        g = Gather(piece, xr_send.at[slot], xr_recv.at[slot])
        g.straight = (stage == 1) & (i == 0)
        return g

    def x_own(i, src):
        slot = lax.rem(i, depth)
        return pltpu.make_async_copy(src, xf.at[slot, rows_of(me, shard)], xr_recv.at[slot, 4 * PARTS + 2])

    def x_copies(i, ref, send, pp):
        g = gather_x(i)
        g.send = send
        return g.near_copies(lambda h, j: x_part(ref, h, j), {"tp": right, "pp": pp}, {"tp": left, "pp": pp})

    def straight_copies():
        g = gather_x(0)
        n = g.parts
        pp = {"tp": opp, "pp": lax.rem(stage + 1, num_stages)}
        return [
            remote(x_part(x2.at[0], h, j), g.piece(me, h, j), st_send.at[h * n + j], g.recv.at[(2 + h) * n + 2 + j], pp)
            for j in range(n)
            for h in range(2)
        ]

    def begin_copies(i):
        return x_copies(i, x_hbm.at[i], xb_send.at[lax.rem(i, depth)], stage)

    def begin(i):
        for c in begin_copies(i):
            c.start()
        x_own(i, x_hbm.at[i]).start()

    def scatter(i, c):
        slot = lax.rem(i, 2)
        cols = cuts[c]

        def copy(k, owner, device):
            return remote(
                part.at[slot, rows_of(owner, shard), cols], fin.at[slot, k, :, cols],
                rs_send.at[slot, c, k], rs_recv.at[slot, c, k], device,
            )

        return copy(2, opp, to_opp), copy(0, right, to_right), copy(1, left, to_left)

    def ln_shard(i, owner):
        at = rows_of(owner, shard)
        nb[at] = norm_rows(xf[lax.rem(i, depth), at], g1_ref[...], s1_ref[...])

    causal = lax.broadcasted_iota(jnp.int32, (seq, seq), 0) >= lax.broadcasted_iota(jnp.int32, (seq, seq), 1)

    def slot_at(s, i):
        even = lax.rem(stage, 2) == 0
        kinds = {"0": stage == 0, "e": even & (stage > 0), "o": ~even}

        def any_of(letter):
            found = [kinds[k] for k in kinds if POINTS[letter + k] == s]
            return functools.reduce(jnp.logical_or, found) if found else None

        h, f, f_first = any_of("H"), any_of("F"), any_of("f")
        if h is not None:
            pl.when(h & (i >= 1))(lambda: hand_on(i - 1))
        go = None
        if f is not None:
            go = f & (i > 0)
        if f_first is not None:
            g = f_first & (i == 0)
            go = g if go is None else go | g
        if go is not None:
            pl.when(go & (i < num_micro - 1))(lambda: gather_x(i + 1).forward())
        if s == 3:
            pl.when((stage == 0) & (i < num_micro - 2))(lambda: begin(i + 2))

    def attention_part(i):
        slot = lax.rem(i, 2)
        gx = gather_x(i)
        x_own(i, x_hbm.at[i]).wait()
        ln_shard(i, me)
        gx.near()
        ln_shard(i, left)
        ln_shard(i, right)
        gx.far()

        @pl.when(stage == 0)
        def _():
            for c in begin_copies(i):
                c.wait_send()

        ln_shard(i, opp)
        for lo, hi in ((0, 768), (768, 1536), (1536, qkv_w)):
            got = jnp.dot(nb[...], wqkv[:, lo:hi], preferred_element_type=F32)
            qkv[:, lo:hi] = (got + bqkv_ref[:, lo:hi]).astype(BF16)
        slot_at(1, i)

        def part_of(n, j):
            at = (3 * n + j) * head_dim
            return qkv[:, at : at + head_dim]

        scores = [
            lax.dot_general(part_of(n, 0), part_of(n, 1), (((1,), (1,)), ((), ())), preferred_element_type=F32)
            for n in range(heads)
        ]
        probs = []
        for s in scores:
            s = jnp.where(causal, s * head_dim**-0.5, -1e30)
            e = jnp.exp(s - jnp.max(s, axis=-1, keepdims=True))
            probs.append((e * (1.0 / jnp.sum(e, axis=-1, keepdims=True))).astype(BF16))
        outs = [jnp.dot(p, part_of(n, 2), preferred_element_type=F32).astype(BF16) for n, p in enumerate(probs)]
        cf[slot, me] = jnp.concatenate(outs, axis=-1)
        gather_c(i).start()

    chunk = 512

    def out_block(i, owner, cols):
        return jnp.dot(cf[lax.rem(i, 2), owner], wout[rows_of(owner, own_k), cols], preferred_element_type=F32)

    def over_columns(f, lo=0, hi=width):
        for at in range(lo, hi, chunk):
            f(pl.ds(at, min(chunk, hi - at)))

    def out_own(i):
        def f(cols):
            acc[:, cols] = out_block(i, me, cols)

        over_columns(f)

    def mlp_first(i):
        slot = lax.rem(i, depth)
        gc = gather_c(i)
        pl.when((stage == 0) & (i == 0))(whole_even.end)
        pl.when((stage == 1) & (i == 0))(whole_odd.end)
        gc.near()

        def near(cols):
            acc[:, cols] = acc[:, cols] + out_block(i, left, cols) + out_block(i, right, cols)

        over_columns(near)
        slot_at(4, i)
        gc.far()

        def far(cols):
            a = (acc[:, cols] + out_block(i, opp, cols)).astype(BF16).astype(F32)
            x1[:, cols] = (xf[slot, :, cols].astype(F32) + a + bout_ref[:, cols]).astype(BF16)

        over_columns(far)
        gc.sent()
        slot_at(5, i)

        @pl.when((stage > 0) & (i < num_micro - depth))
        def _():
            for k, device in zip((0, 2, 1), beside(stage - 1)):
                signal(free_sem.at[k], device)

        for r in range(ring):
            at = pl.ds(r * shard, shard)
            nb[at] = norm_rows(x1[at], g2_ref[...], s2_ref[...])

        def up(cols):
            got = jnp.dot(nb[...], wup[:, cols], preferred_element_type=F32) + bup_ref[:, cols]
            hid[:, cols] = jnp.maximum(got, 0.0).astype(BF16)

        over_columns(up)

    def mlp_second(i):
        slot = lax.rem(i, 2)

        def down(cols):
            part[slot, :, cols] = jnp.dot(hid[...], wdn[:, cols], preferred_element_type=F32).astype(BF16)

        for c in range(len(cuts)):
            over_columns(down, cuts[c].start, cuts[c].start + cuts[c].size)
            for copy in scatter(i, c):
                copy.start()
            if c == 0:
                slot_at(7, i)

    def next_copies(i):
        slot = lax.rem(i, 2)
        send = pp_send.at[slot]
        pp = lax.rem(stage + 1, num_stages)
        own = remote(
            x2.at[slot], xf.at[lax.rem(i, depth), rows_of(me, shard)], send.at[2 * PARTS + 2],
            xr_recv.at[lax.rem(i, depth), 4 * PARTS + 2], {"pp": pp},
        )
        return *x_copies(i, x2.at[slot], send, pp), own

    def out_copy(i):
        slot = lax.rem(i, 2)
        at = lax.rem(i, per_stage)
        return remote(x2.at[slot], obuf.at[at], pp_send.at[slot, 2 * PARTS + 2], o_sem.at[at], {"pp": i // per_stage})

    def sent_on(i):
        @pl.when(stage < last)
        def _():
            for c in next_copies(i):
                c.wait_send()

            @pl.when((stage == 0) & (i == 0))
            def _():
                for c in straight_copies():
                    c.wait_send()

        pl.when((stage == last) & (i < per_stage * last))(lambda: out_copy(i).wait_send())

    def later(i):
        return (lax.rem(stage, 2) == 0) & (i < num_micro - 1)

    def hand_on_rest(i):
        @pl.when((stage < last) & later(i))
        def _():
            for c in next_copies(i)[2 * PARTS :]:
                c.start()

    def hand_on(i):
        slot = lax.rem(i, 2)
        pl.when(i >= 2)(lambda: sent_on(i - 2))
        own = rows_of(me, shard)
        for c in range(len(cuts)):
            copies = scatter(i, c)
            for copy in copies:
                copy.wait_recv()
            cols = cuts[c]
            m = part[slot, own, cols].astype(F32)
            for k in range(3):
                m = m + fin[slot, k, :, cols].astype(F32)
            m = m.astype(BF16).astype(F32)
            x2[slot, :, cols] = (x1[own, cols].astype(F32) + m + bdn_ref[:, cols]).astype(BF16)

        @pl.when(stage < last)
        def _():
            @pl.when(i >= depth)
            def _():
                for k in range(3):
                    pl.semaphore_wait(free_sem.at[k], 1)

            @pl.when((stage == 0) & (i == 0))
            def _():
                for c in straight_copies():
                    c.start()

            copies = next_copies(i)
            for c in copies[: 2 * PARTS]:
                c.start()

            @pl.when(~later(i))
            def _():
                for c in copies[2 * PARTS :]:
                    c.start()

        pl.when((stage == last) & (i < per_stage * last))(lambda: out_copy(i).start())

        @pl.when((stage == last) & (i >= per_stage * last))
        def _():
            obuf[lax.rem(i, per_stage)] = x2[slot]

        for c in range(len(cuts)):
            for copy in scatter(i, c):
                copy.wait_send()

    load_out.wait()
    even = lax.rem(stage, 2) == 0

    @pl.when(stage == 0)
    def _():
        begin(0)
        whole_even.lend_all()
        gather_x(0).forward()
        whole_even.first.start()
        begin(1)
        whole_even.lent_all()
        signal(turn_sem.at[1], {"pp": stage + 1})

    @pl.when(stage == 1)
    def _():
        pl.semaphore_wait(turn_sem.at[1], 1)
        whole_odd.lend_all()
        pl.semaphore_wait(turn_sem.at[0], 1)
        whole_odd.first.start()
        whole_odd.first.forward()
        whole_odd.lent_all()

    @pl.when((stage > 1) & even)
    def _():
        w = whole_even
        for p in range(2):
            pl.when(helps(p))(lambda p=p: w.help_gather(p, True))
        for g in (w.first, w.rest):
            g.start()

        @pl.when(helps(0) | helps(1))
        def _():
            for p in range(2):
                pl.when(helps(p))(lambda p=p: w.help_end(p))
            load_dn.start()
            signal(turn_sem.at[2], {"pp": stage + 1})

        for g in (w.first, w.rest):
            g.forward()
        for g in (w.first, w.rest):
            g.finish()
        signal(turn_sem.at[0], {"pp": stage + 1})

    @pl.when((stage > 1) & ~even)
    def _():
        w = whole_odd
        pl.when(stage == 3)(w.lend_all)
        pl.when(stage == 3)(lambda: w.help_gather(1, False))
        pl.when(stage == last)(lambda: w.help_gather(0, False))

        @pl.when(stage == 5)
        def _():
            for p in range(2):
                w.help_gather(p, True)

        pl.semaphore_wait(turn_sem.at[0], 1)
        w.first.start()
        pl.when(stage != 3)(w.rest.start)
        for p in range(2):
            pl.when(helps(p))(lambda p=p: w.help_end(p))
        load_dn.start()
        w.first.forward()

        @pl.when(stage != 3)
        def _():
            w.rest.forward()
            w.first.finish()
            w.rest.finish()

        @pl.when(stage == 3)
        def _():
            w.lent_all()
            w.end()

    load_qkv.wait()
    load_up.wait()
    load_dn.wait()
    pl.when(stage > 0)(lambda: gather_x(0).forward())

    def step(i, carry):
        here = i < num_micro

        @pl.when(here)
        def _():
            slot_at(0, i)
            attention_part(i)
            out_own(i)

            @pl.when((stage == 0) & (i == 0))
            def _():
                whole_even.first.forward()

            slot_at(2, i)

        pl.when(i == num_micro)(lambda: hand_on(i - 1))

        @pl.when(here)
        def _():
            gather_c(i).forward()
            pl.when(i >= 1)(lambda: hand_on_rest(i - 1))
            slot_at(3, i)
            mlp_first(i)
            slot_at(6, i)
            mlp_second(i)
            slot_at(8, i)

        return carry

    lax.fori_loop(0, num_micro + 1, step, 0)

    for i in range(num_micro - 2, num_micro):
        sent_on(i)

    @pl.when(stage < last)
    def _():
        for j in range(per_stage):
            out_copy(j).wait_recv()

    out_ref[...] = obuf[...]


def solution(mesh):
    num_stages = mesh.shape["pp"]
    ring = mesh.shape["tp"]
    in_specs = (P("dp", None, "tp", None),
                P("pp", None), P("pp", None), P("pp", None, "tp"), P("pp", "tp"),
                P("pp", "tp", None, None), P("pp", None), P("pp", None), P("pp", None),
                P("pp", None, "tp"), P("pp", "tp"), P("pp", "tp", None), P("pp", None))
    out_specs = P(("dp", "pp"), None, "tp", None)

    def device_program(x_local, g1, s1, w_qkv, b_qkv, w_out, b_out, g2, s2, w_up, b_up, w_down, b_down):
        num_micro, batch, shard, width = x_local.shape
        local_heads, head_dim = w_out.shape[1], w_out.shape[2]
        own_k = local_heads * head_dim
        qkv_w, ff = w_qkv.shape[2], w_up.shape[2]
        rows = batch * shard
        seq = rows * ring
        per_stage = num_micro // num_stages
        hbm = pl.BlockSpec(memory_space=pl.ANY)
        vmem = pl.BlockSpec(memory_space=pltpu.VMEM)
        dma = pltpu.SemaphoreType.DMA
        out = pl.pallas_call(
            functools.partial(layer_kernel, num_stages, ring, head_dim),
            name="layers",
            out_shape=jax.ShapeDtypeStruct((per_stage, rows, width), BF16),
            in_specs=[hbm, vmem, vmem, hbm, vmem, hbm, vmem, vmem, vmem, hbm, vmem, hbm, vmem],
            out_specs=vmem,
            scratch_shapes=[
                pltpu.VMEM((width, qkv_w), BF16),
                pltpu.VMEM((own_k * ring, width), BF16),
                pltpu.VMEM((width, ff), BF16),
                pltpu.VMEM((ff, width), BF16),
                pltpu.VMEM((4, seq, width), BF16),
                pltpu.VMEM((seq, width), BF16),
                pltpu.VMEM((seq, qkv_w), BF16),
                pltpu.VMEM((2, ring, seq, own_k), BF16),
                pltpu.VMEM((seq, width), F32),
                pltpu.VMEM((seq, width), BF16),
                pltpu.VMEM((seq, ff), BF16),
                pltpu.VMEM((2, seq, width), BF16),
                pltpu.VMEM((2, 3, rows, width), BF16),
                pltpu.VMEM((2, rows, width), BF16),
                pltpu.VMEM((per_stage, rows, width), BF16),
                dma((4,)),
                dma((2, 6)),
                dma((2, 6)),
                dma((2, 6)),
                dma((2, 6)),
                dma((2, 2)),
                dma((2, 2)),
                dma((2, 6)),
                dma((2, 6)),
                dma((4, 2 * PARTS + 2)),
                dma((4, 4 * PARTS + 2)),
                dma((4, 4 * PARTS + 3)),
                dma((2, 4 * PARTS + 2)),
                dma((2, 4 * PARTS + 2)),
                dma((2, len(CUT_FIFTHS), 3)),
                dma((2, len(CUT_FIFTHS), 3)),
                dma((2 * PARTS,)),
                dma((2, 2 * PARTS + 3)),
                dma((per_stage,)),
                pltpu.SemaphoreType.REGULAR((3,)),
                pltpu.SemaphoreType.REGULAR((3,)),
            ],
            compiler_params=pltpu.CompilerParams(
                collective_id=0, has_side_effects=True, vmem_limit_bytes=67_043_328
            ),
        )(
            x_local.reshape(num_micro, rows, width), g1, s1, w_qkv[0], b_qkv, w_out.reshape(own_k, width), b_out,
            g2, s2, w_up[0], b_up, w_down[0], b_down,
        )
        return out.reshape(per_stage, batch, shard, width)

    return jax.shard_map(device_program, mesh=mesh, in_specs=in_specs, out_specs=out_specs, check_vma=False)
```

```python
import functools

import jax
import jax.numpy as jnp
from jax import lax
from jax.experimental import pallas as pl
from jax.experimental.pallas import tpu as pltpu
from jax.sharding import PartitionSpec as P

LN_EPS = 1e-5
MESH = pl.DeviceIdType.MESH
PARTS = 2
CUT_FIFTHS = (1, 1, 1, 2)
POINTS = {"H0": 2, "He": 2, "Ho": 2, "F0": 6, "Fe": 5, "Fo": 6, "f0": 6, "fe": 6, "fo": 6}
F32 = jnp.float32
BF16 = jnp.bfloat16


def norm_rows(rows, gain, shift):
    rows = rows.astype(F32)
    centered = rows - jnp.mean(rows, axis=-1, keepdims=True)
    var = jnp.mean(centered * centered, axis=-1, keepdims=True)
    return (centered * lax.rsqrt(var + LN_EPS) * gain + shift).astype(BF16)


def layer_kernel(
    num_stages, ring, head_dim,
    x_hbm, g1_ref, s1_ref, wqkv_hbm, bqkv_ref, wout_hbm, bout_ref,
    g2_ref, s2_ref, wup_hbm, bup_ref, wdn_hbm, bdn_ref,
    out_ref,
    wqkv, wout, wup, wdn,
    xf, nb, qkv, cf, acc, x1, hid, part, fin, x2, obuf,
    w_sem, wg_send, wg_recv, wh_send, wh_recv, wx_send, wx_recv, wr_send, wr_recv, xb_send, xr_send, xr_recv, ac_send, ac_recv,
    rs_send, rs_recv, st_send, pp_send, o_sem, turn_sem, free_sem,
):
    num_micro, shard, width = x_hbm.shape
    seq = shard * ring
    per_stage = num_micro // num_stages
    own_k = wout_hbm.shape[0]
    qkv_w = wqkv_hbm.shape[1]
    heads = own_k // head_dim
    fifth = width // 5
    cuts = tuple(pl.ds(sum(CUT_FIFTHS[:c]) * fifth, n * fifth) for c, n in enumerate(CUT_FIFTHS))
    last = num_stages - 1
    depth = xf.shape[0]

    me = lax.axis_index("tp")
    stage = lax.axis_index("pp")
    right = lax.rem(me + 1, ring)
    left = lax.rem(me + ring - 1, ring)
    opp = lax.rem(me + 2, ring)
    to_right, to_left, to_opp = {"tp": right}, {"tp": left}, {"tp": opp}

    def rows_of(owner, n):
        return pl.ds(pl.multiple_of(owner * n, n), n)

    def remote(src, dst, send, recv, device):
        return pltpu.make_async_remote_copy(
            src_ref=src, dst_ref=dst, send_sem=send, recv_sem=recv, device_id=device, device_id_type=MESH
        )

    def signal(sem, device):
        pl.semaphore_signal(sem, inc=1, device_id=device, device_id_type=MESH)

    lends = (stage < 2) | (stage == 3)

    def helper(p):
        return stage + (jnp.where(stage == 3, 2, last - 1), 2)[p]

    def helped(p):
        return stage - (jnp.where(stage == 5, 2, last - 1), 2)[p]

    def helps(p):
        return ((stage >= last - 1) | (stage == 5), (stage == 2) | (stage == 3) | (stage == 5))[p]

    barrier = pltpu.get_barrier_semaphore()

    def beside(pp):
        return ({"pp": pp}, {"tp": right, "pp": pp}, {"tp": left, "pp": pp})

    for device in (to_right, to_left, to_opp):
        signal(barrier, device)

    @pl.when(stage > 0)
    def _():
        for device in beside(stage - 1):
            signal(barrier, device)

    @pl.when(stage < last)
    def _():
        for device in beside(stage + 1):
            signal(barrier, device)

    pl.when(stage < last - 1)(lambda: signal(barrier, {"pp": last}))

    for here, there in ((0, 1), (1, 0)):
        pl.when(stage == here)(lambda there=there: signal(barrier, {"tp": opp, "pp": there}))

    @pl.when(lends)
    def _():
        for p in range(2):
            signal(barrier, {"pp": helper(p)})

    pl.when(helps(0))(lambda: signal(barrier, {"pp": helped(0)}))
    pl.when(helps(1))(lambda: signal(barrier, {"pp": helped(1)}))

    @pl.when(stage == last)
    def _():
        for q in range(last - 1):
            signal(barrier, {"pp": q})

    load_out = pltpu.make_async_copy(wout_hbm, wout.at[rows_of(me, own_k)], w_sem.at[0])
    load_qkv = pltpu.make_async_copy(wqkv_hbm, wqkv, w_sem.at[1])
    load_up = pltpu.make_async_copy(wup_hbm, wup, w_sem.at[2])
    load_dn = pltpu.make_async_copy(wdn_hbm, wdn, w_sem.at[3])
    load_out.start()
    load_qkv.start()
    load_up.start()
    pl.when(~(helps(0) | helps(1)))(load_dn.start)

    pl.semaphore_wait(
        barrier,
        3
        + jnp.where(stage > 0, 3, 0)
        + jnp.where(stage < last, 3, 0)
        + jnp.where(stage < last - 1, 1, 0)
        + jnp.where(stage == last, last - 1, 0)
        + jnp.where(stage < 2, 1, 0)
        + jnp.where(lends, 2, 0)
        + jnp.where(helps(0), 1, 0)
        + jnp.where(helps(1), 1, 0),
    )

    class Gather:
        def __init__(self, piece, send, recv, parts=PARTS):
            self.piece, self.send, self.recv, self.parts = piece, send, recv, parts
            self.straight = None

        def copy(self, k, src, dst, device):
            return remote(src, dst, self.send.at[k], self.recv.at[k], device)

        def near_copies(self, src, right_device, left_device):
            n = self.parts
            first = []
            for j in range(n):
                first.append(self.copy(j, src(0, j), self.piece(me, 0, j), right_device))
                first.append(self.copy(n + j, src(1, j), self.piece(me, 1, j), left_device))
            return (
                *first,
                self.copy(2 * n, src(1, None), self.piece(me, 1, None), right_device),
                self.copy(2 * n + 1, src(0, None), self.piece(me, 0, None), left_device),
            )

        def hop1(self):
            return self.near_copies(lambda h, j: self.piece(me, h, j), to_right, to_left)

        def fwd(self):
            n = self.parts
            pairs = []
            for j in range(n):
                pairs.append((j, self.copy(2 * n + 2 + j, self.piece(left, 0, j), self.piece(left, 0, j), to_right)))
                pairs.append((n + j, self.copy(3 * n + 2 + j, self.piece(right, 1, j), self.piece(right, 1, j), to_left)))
            return pairs

        def start(self):
            for c in self.hop1():
                c.start()

        def arrived(self, k, owner, h, j):
            self.copy(k, self.piece(owner, h, j), self.piece(owner, h, j), to_right).wait_recv()

        def forward(self):
            n = self.parts
            for k, c in self.fwd():
                self.arrived(k, *((left, 0, k) if k < n else (right, 1, k - n)))
                c.start() if self.straight is None else pl.when(~self.straight)(c.start)

        def near(self):
            n = self.parts
            self.arrived(2 * n, left, 1, None)
            self.arrived(2 * n + 1, right, 0, None)

        def far(self):
            n = self.parts
            for j in range(n):
                self.arrived(2 * n + 2 + j, opp, 0, j)
                self.arrived(3 * n + 2 + j, opp, 1, j)

            def forwarded():
                for _, c in self.fwd():
                    c.wait_send()

            forwarded() if self.straight is None else pl.when(~self.straight)(forwarded)

        def sent(self):
            for c in self.hop1():
                c.wait_send()

        def finish(self):
            self.near()
            self.far()
            self.sent()

    class Whole:
        def __init__(self, by_y, by_x):
            self.by_y, self.by_x = by_y, by_x
            self.first = Gather(self.piece(0, by_y), wg_send.at[0], wg_recv.at[0], 1)
            self.rest = Gather(self.piece(by_y, 2 * by_x), wg_send.at[1], wg_recv.at[1], 1)

        @staticmethod
        def half_of(n, h):
            first = -(-n // 32) * 16
            return (0, first) if h == 0 else (first, n - first)

        def piece(self, lo, n):
            def of(owner, h, j=None):
                at, size = self.half_of(n, h)
                return wout.at[pl.ds(pl.multiple_of(owner * own_k + lo + at, 16), size)]

            return of

        def path(self, p):
            return self.piece(self.by_y + p * self.by_x, self.by_x)

        def lent(self, p):
            def of(owner, h, j=None):
                at, size = self.half_of(self.by_x, h)
                return wdn.at[pl.ds(pl.multiple_of((p * ring + owner) * self.by_x + at, 16), size)]

            return of

        def lend(self, p, h, pp):
            return remote(self.path(p)(me, h), self.lent(p)(me, h), wx_send.at[p, h], wx_recv.at[p, h], {"pp": pp})

        def give_back(self, p, k, pp):
            owner, h = others[k]
            return remote(
                self.lent(p)(owner, h), self.path(p)(owner, h), wr_send.at[p, k], wr_recv.at[p, k], {"pp": pp}
            )

        def helper_ring(self, p):
            return Gather(self.lent(p), wh_send.at[p], wh_recv.at[p], 1)

        def help_gather(self, p, now):
            pp, g = helped(p), self.helper_ring(p)
            for h in range(2):
                self.lend(p, h, pp).wait_recv()
                for c in (g.hop1()[0], g.hop1()[3]) if h == 0 else (g.hop1()[1], g.hop1()[2]):
                    c.start()
            for k in range(6):
                g.arrived(k, *others[k], None)
                if k < 2:
                    g.fwd()[k][1].start()
                if now:
                    self.give_back(p, k, pp).start()
            if not now:
                pl.semaphore_wait(turn_sem.at[2], 1)
                for k in range(6):
                    self.give_back(p, k, pp).start()

        def help_end(self, p):
            g = self.helper_ring(p)
            g.sent()
            for _, c in g.fwd():
                c.wait_send()
            for k in range(6):
                self.give_back(p, k, helped(p)).wait_send()

        def lend_all(self):
            for h in range(2):
                for p in range(2):
                    self.lend(p, h, helper(p)).start()

        def lent_all(self):
            for h in range(2):
                for p in range(2):
                    self.lend(p, h, helper(p)).wait_send()

        def end(self):
            self.first.finish()
            pl.when(stage == 0)(lambda: signal(turn_sem.at[0], {"pp": stage + 1}))
            for p in range(2):
                for k in range(6):
                    self.give_back(p, k, helper(p)).wait_recv()

    others = ((left, 0), (right, 1), (left, 1), (right, 0), (opp, 0), (opp, 1))
    whole_even = Whole(own_k // 2, own_k // 4)
    whole_odd = Whole(9 * own_k // 20, 11 * own_k // 40)

    def gather_c(i):
        slot = lax.rem(i, 2)
        ch = seq // 2
        cn = ch // PARTS

        def piece(owner, h, j=None):
            rows = pl.ds(h * ch, ch) if j is None else pl.ds(h * ch + j * cn, cn)
            return cf.at[slot, owner, rows]

        return Gather(piece, ac_send.at[slot], ac_recv.at[slot])

    xh = shard // 2

    xn = width // PARTS

    def x_part(ref, h, j):
        at = pl.ds(h * xh, xh)
        return ref.at[at] if j is None else ref.at[at, pl.ds(j * xn, xn)]

    def gather_x(i):
        slot = lax.rem(i, depth)

        def piece(owner, h, j=None):
            at = pl.ds(pl.multiple_of(owner * shard + h * xh, xh), xh)
            return xf.at[slot, at] if j is None else xf.at[slot, at, pl.ds(j * xn, xn)]

        g = Gather(piece, xr_send.at[slot], xr_recv.at[slot])
        g.straight = (stage == 1) & (i == 0)
        return g

    def x_own(i, src):
        slot = lax.rem(i, depth)
        return pltpu.make_async_copy(src, xf.at[slot, rows_of(me, shard)], xr_recv.at[slot, 4 * PARTS + 2])

    def x_copies(i, ref, send, pp):
        g = gather_x(i)
        g.send = send
        return g.near_copies(lambda h, j: x_part(ref, h, j), {"tp": right, "pp": pp}, {"tp": left, "pp": pp})

    def straight_copies():
        g = gather_x(0)
        n = g.parts
        pp = {"tp": opp, "pp": lax.rem(stage + 1, num_stages)}
        return [
            remote(x_part(x2.at[0], h, j), g.piece(me, h, j), st_send.at[h * n + j], g.recv.at[(2 + h) * n + 2 + j], pp)
            for j in range(n)
            for h in range(2)
        ]

    def begin_copies(i):
        return x_copies(i, x_hbm.at[i], xb_send.at[lax.rem(i, depth)], stage)

    def begin(i):
        for c in begin_copies(i):
            c.start()
        x_own(i, x_hbm.at[i]).start()

    def scatter(i, c):
        slot = lax.rem(i, 2)
        cols = cuts[c]

        def copy(k, owner, device):
            return remote(
                part.at[slot, rows_of(owner, shard), cols], fin.at[slot, k, :, cols],
                rs_send.at[slot, c, k], rs_recv.at[slot, c, k], device,
            )

        return copy(2, opp, to_opp), copy(0, right, to_right), copy(1, left, to_left)

    def ln_shard(i, owner):
        at = rows_of(owner, shard)
        nb[at] = norm_rows(xf[lax.rem(i, depth), at], g1_ref[...], s1_ref[...])

    causal = lax.broadcasted_iota(jnp.int32, (seq, seq), 0) >= lax.broadcasted_iota(jnp.int32, (seq, seq), 1)

    def slot_at(s, i):
        even = lax.rem(stage, 2) == 0
        kinds = {"0": stage == 0, "e": even & (stage > 0), "o": ~even}

        def any_of(letter):
            found = [kinds[k] for k in kinds if POINTS[letter + k] == s]
            return functools.reduce(jnp.logical_or, found) if found else None

        h, f, f_first = any_of("H"), any_of("F"), any_of("f")
        if h is not None:
            pl.when(h & (i >= 1))(lambda: hand_on(i - 1))
        go = None
        if f is not None:
            go = f & (i > 0)
        if f_first is not None:
            g = f_first & (i == 0)
            go = g if go is None else go | g
        if go is not None:
            pl.when(go & (i < num_micro - 1))(lambda: gather_x(i + 1).forward())
        if s == 3:
            pl.when((stage == 0) & (i < num_micro - 2))(lambda: begin(i + 2))

    def attention_part(i):
        slot = lax.rem(i, 2)
        gx = gather_x(i)
        x_own(i, x_hbm.at[i]).wait()
        ln_shard(i, me)
        gx.near()
        ln_shard(i, left)
        ln_shard(i, right)
        gx.far()

        @pl.when(stage == 0)
        def _():
            for c in begin_copies(i):
                c.wait_send()

        ln_shard(i, opp)
        for lo, hi in ((0, 768), (768, 1536), (1536, qkv_w)):
            got = jnp.dot(nb[...], wqkv[:, lo:hi], preferred_element_type=F32)
            qkv[:, lo:hi] = (got + bqkv_ref[:, lo:hi]).astype(BF16)
        slot_at(1, i)

        def part_of(n, j):
            at = (3 * n + j) * head_dim
            return qkv[:, at : at + head_dim]

        scores = [
            lax.dot_general(part_of(n, 0), part_of(n, 1), (((1,), (1,)), ((), ())), preferred_element_type=F32)
            for n in range(heads)
        ]
        probs = []
        for s in scores:
            s = jnp.where(causal, s * head_dim**-0.5, -1e30)
            e = jnp.exp(s - jnp.max(s, axis=-1, keepdims=True))
            probs.append((e * (1.0 / jnp.sum(e, axis=-1, keepdims=True))).astype(BF16))
        outs = [jnp.dot(p, part_of(n, 2), preferred_element_type=F32).astype(BF16) for n, p in enumerate(probs)]
        cf[slot, me] = jnp.concatenate(outs, axis=-1)
        gather_c(i).start()

    chunk = 512

    def out_block(i, owner, cols):
        return jnp.dot(cf[lax.rem(i, 2), owner], wout[rows_of(owner, own_k), cols], preferred_element_type=F32)

    def over_columns(f, lo=0, hi=width):
        for at in range(lo, hi, chunk):
            f(pl.ds(at, min(chunk, hi - at)))

    def out_own(i):
        def f(cols):
            acc[:, cols] = out_block(i, me, cols)

        over_columns(f)

    def mlp_first(i):
        slot = lax.rem(i, depth)
        gc = gather_c(i)
        pl.when((stage == 0) & (i == 0))(whole_even.end)
        pl.when((stage == 1) & (i == 0))(whole_odd.end)
        gc.near()

        def near(cols):
            acc[:, cols] = acc[:, cols] + out_block(i, left, cols) + out_block(i, right, cols)

        over_columns(near)
        slot_at(4, i)
        gc.far()

        def far(cols):
            a = (acc[:, cols] + out_block(i, opp, cols)).astype(BF16).astype(F32)
            x1[:, cols] = (xf[slot, :, cols].astype(F32) + a + bout_ref[:, cols]).astype(BF16)

        over_columns(far)
        gc.sent()
        slot_at(5, i)

        @pl.when((stage > 0) & (i < num_micro - depth))
        def _():
            for k, device in zip((0, 2, 1), beside(stage - 1)):
                signal(free_sem.at[k], device)

        for r in range(ring):
            at = pl.ds(r * shard, shard)
            nb[at] = norm_rows(x1[at], g2_ref[...], s2_ref[...])

        def up(cols):
            got = jnp.dot(nb[...], wup[:, cols], preferred_element_type=F32) + bup_ref[:, cols]
            hid[:, cols] = jnp.maximum(got, 0.0).astype(BF16)

        over_columns(up)

    def mlp_second(i):
        slot = lax.rem(i, 2)

        def down(cols):
            part[slot, :, cols] = jnp.dot(hid[...], wdn[:, cols], preferred_element_type=F32).astype(BF16)

        for c in range(len(cuts)):
            over_columns(down, cuts[c].start, cuts[c].start + cuts[c].size)
            for copy in scatter(i, c):
                copy.start()
            if c == 0:
                slot_at(7, i)

    def next_copies(i):
        slot = lax.rem(i, 2)
        send = pp_send.at[slot]
        pp = lax.rem(stage + 1, num_stages)
        own = remote(
            x2.at[slot], xf.at[lax.rem(i, depth), rows_of(me, shard)], send.at[2 * PARTS + 2],
            xr_recv.at[lax.rem(i, depth), 4 * PARTS + 2], {"pp": pp},
        )
        return *x_copies(i, x2.at[slot], send, pp), own

    def out_copy(i):
        slot = lax.rem(i, 2)
        at = lax.rem(i, per_stage)
        return remote(x2.at[slot], obuf.at[at], pp_send.at[slot, 2 * PARTS + 2], o_sem.at[at], {"pp": i // per_stage})

    def sent_on(i):
        @pl.when(stage < last)
        def _():
            for c in next_copies(i):
                c.wait_send()

            @pl.when((stage == 0) & (i == 0))
            def _():
                for c in straight_copies():
                    c.wait_send()

        pl.when((stage == last) & (i < per_stage * last))(lambda: out_copy(i).wait_send())

    def later(i):
        return (lax.rem(stage, 2) == 0) & (i < num_micro - 1)

    def hand_on_rest(i):
        @pl.when((stage < last) & later(i))
        def _():
            for c in next_copies(i)[2 * PARTS :]:
                c.start()

    def hand_on(i):
        slot = lax.rem(i, 2)
        pl.when(i >= 2)(lambda: sent_on(i - 2))
        own = rows_of(me, shard)
        for c in range(len(cuts)):
            copies = scatter(i, c)
            for copy in copies:
                copy.wait_recv()
            cols = cuts[c]
            m = part[slot, own, cols].astype(F32)
            for k in range(3):
                m = m + fin[slot, k, :, cols].astype(F32)
            m = m.astype(BF16).astype(F32)
            x2[slot, :, cols] = (x1[own, cols].astype(F32) + m + bdn_ref[:, cols]).astype(BF16)

        @pl.when(stage < last)
        def _():
            @pl.when(i >= depth)
            def _():
                for k in range(3):
                    pl.semaphore_wait(free_sem.at[k], 1)

            @pl.when((stage == 0) & (i == 0))
            def _():
                for c in straight_copies():
                    c.start()

            copies = next_copies(i)
            for c in copies[: 2 * PARTS]:
                c.start()

            @pl.when(~later(i))
            def _():
                for c in copies[2 * PARTS :]:
                    c.start()

        pl.when((stage == last) & (i < per_stage * last))(lambda: out_copy(i).start())

        @pl.when((stage == last) & (i >= per_stage * last))
        def _():
            obuf[lax.rem(i, per_stage)] = x2[slot]

        for c in range(len(cuts)):
            for copy in scatter(i, c):
                copy.wait_send()

    load_out.wait()
    even = lax.rem(stage, 2) == 0

    @pl.when(stage == 0)
    def _():
        begin(0)
        whole_even.lend_all()
        gather_x(0).forward()
        whole_even.first.start()
        begin(1)
        whole_even.lent_all()
        signal(turn_sem.at[1], {"pp": stage + 1})

    @pl.when(stage == 1)
    def _():
        pl.semaphore_wait(turn_sem.at[1], 1)
        whole_odd.lend_all()
        pl.semaphore_wait(turn_sem.at[0], 1)
        whole_odd.first.start()
        whole_odd.first.forward()
        whole_odd.lent_all()

    @pl.when((stage > 1) & even)
    def _():
        w = whole_even
        for p in range(2):
            pl.when(helps(p))(lambda p=p: w.help_gather(p, True))
        for g in (w.first, w.rest):
            g.start()

        @pl.when(helps(0) | helps(1))
        def _():
            for p in range(2):
                pl.when(helps(p))(lambda p=p: w.help_end(p))
            load_dn.start()
            signal(turn_sem.at[2], {"pp": stage + 1})

        for g in (w.first, w.rest):
            g.forward()
        for g in (w.first, w.rest):
            g.finish()
        signal(turn_sem.at[0], {"pp": stage + 1})

    @pl.when((stage > 1) & ~even)
    def _():
        w = whole_odd
        pl.when(stage == 3)(w.lend_all)
        pl.when(stage == 3)(lambda: w.help_gather(1, False))
        pl.when(stage == last)(lambda: w.help_gather(0, False))

        @pl.when(stage == 5)
        def _():
            for p in range(2):
                w.help_gather(p, True)

        pl.semaphore_wait(turn_sem.at[0], 1)
        w.first.start()
        pl.when(stage != 3)(w.rest.start)
        for p in range(2):
            pl.when(helps(p))(lambda p=p: w.help_end(p))
        load_dn.start()
        w.first.forward()

        @pl.when(stage != 3)
        def _():
            w.rest.forward()
            w.first.finish()
            w.rest.finish()

        @pl.when(stage == 3)
        def _():
            w.lent_all()
            w.end()

    load_qkv.wait()
    load_up.wait()
    load_dn.wait()
    pl.when(stage > 0)(lambda: gather_x(0).forward())

    def step(i, carry):
        here = i < num_micro

        @pl.when(here)
        def _():
            slot_at(0, i)
            attention_part(i)
            out_own(i)

            @pl.when((stage == 0) & (i == 0))
            def _():
                whole_even.first.forward()

            slot_at(2, i)

        pl.when(i == num_micro)(lambda: hand_on(i - 1))

        @pl.when(here)
        def _():
            gather_c(i).forward()
            pl.when(i >= 1)(lambda: hand_on_rest(i - 1))
            slot_at(3, i)
            mlp_first(i)
            slot_at(6, i)
            mlp_second(i)
            slot_at(8, i)

        return carry

    lax.fori_loop(0, num_micro + 1, step, 0)

    for i in range(num_micro - 2, num_micro):
        sent_on(i)

    @pl.when(stage < last)
    def _():
        for j in range(per_stage):
            out_copy(j).wait_recv()

    out_ref[...] = obuf[...]


def solution(mesh):
    num_stages = mesh.shape["pp"]
    ring = mesh.shape["tp"]
    in_specs = (P("dp", None, "tp", None),
                P("pp", None), P("pp", None), P("pp", None, "tp"), P("pp", "tp"),
                P("pp", "tp", None, None), P("pp", None), P("pp", None), P("pp", None),
                P("pp", None, "tp"), P("pp", "tp"), P("pp", "tp", None), P("pp", None))
    out_specs = P(("dp", "pp"), None, "tp", None)

    def device_program(x_local, g1, s1, w_qkv, b_qkv, w_out, b_out, g2, s2, w_up, b_up, w_down, b_down):
        num_micro, batch, shard, width = x_local.shape
        local_heads, head_dim = w_out.shape[1], w_out.shape[2]
        own_k = local_heads * head_dim
        qkv_w, ff = w_qkv.shape[2], w_up.shape[2]
        rows = batch * shard
        seq = rows * ring
        per_stage = num_micro // num_stages
        hbm = pl.BlockSpec(memory_space=pl.ANY)
        vmem = pl.BlockSpec(memory_space=pltpu.VMEM)
        dma = pltpu.SemaphoreType.DMA
        out = pl.pallas_call(
            functools.partial(layer_kernel, num_stages, ring, head_dim),
            name="layers",
            out_shape=jax.ShapeDtypeStruct((per_stage, rows, width), BF16),
            in_specs=[hbm, vmem, vmem, hbm, vmem, hbm, vmem, vmem, vmem, hbm, vmem, hbm, vmem],
            out_specs=vmem,
            scratch_shapes=[
                pltpu.VMEM((width, qkv_w), BF16),
                pltpu.VMEM((own_k * ring, width), BF16),
                pltpu.VMEM((width, ff), BF16),
                pltpu.VMEM((ff, width), BF16),
                pltpu.VMEM((4, seq, width), BF16),
                pltpu.VMEM((seq, width), BF16),
                pltpu.VMEM((seq, qkv_w), BF16),
                pltpu.VMEM((2, ring, seq, own_k), BF16),
                pltpu.VMEM((seq, width), F32),
                pltpu.VMEM((seq, width), BF16),
                pltpu.VMEM((seq, ff), BF16),
                pltpu.VMEM((2, seq, width), BF16),
                pltpu.VMEM((2, 3, rows, width), BF16),
                pltpu.VMEM((2, rows, width), BF16),
                pltpu.VMEM((per_stage, rows, width), BF16),
                dma((4,)),
                dma((2, 6)),
                dma((2, 6)),
                dma((2, 6)),
                dma((2, 6)),
                dma((2, 2)),
                dma((2, 2)),
                dma((2, 6)),
                dma((2, 6)),
                dma((4, 2 * PARTS + 2)),
                dma((4, 4 * PARTS + 2)),
                dma((4, 4 * PARTS + 3)),
                dma((2, 4 * PARTS + 2)),
                dma((2, 4 * PARTS + 2)),
                dma((2, len(CUT_FIFTHS), 3)),
                dma((2, len(CUT_FIFTHS), 3)),
                dma((2 * PARTS,)),
                dma((2, 2 * PARTS + 3)),
                dma((per_stage,)),
                pltpu.SemaphoreType.REGULAR((3,)),
                pltpu.SemaphoreType.REGULAR((3,)),
            ],
            compiler_params=pltpu.CompilerParams(
                collective_id=0, has_side_effects=True, vmem_limit_bytes=67_043_328
            ),
        )(
            x_local.reshape(num_micro, rows, width), g1, s1, w_qkv[0], b_qkv, w_out.reshape(own_k, width), b_out,
            g2, s2, w_up[0], b_up, w_down[0], b_down,
        )
        return out.reshape(per_stage, batch, shard, width)

    return jax.shard_map(device_program, mesh=mesh, in_specs=in_specs, out_specs=out_specs, check_vma=False)
```
